16 devices in a mesh: data: 16 (over z, y, x, core).
Axes of the slice: x: 2, y: 2, z: 2, core: 2. Of those that a mesh axis runs over, the one named last changes fastest.
Arguments:
- grad_qkv: bfloat16 [16, 3, 1769472], P('data')
- weight_qkv: float32 [3, 1769472], P(None, 'data')
- mom_qkv: float32 [3, 1769472], P(None, 'data')
- var_qkv: float32 [3, 1769472], P(None, 'data')
- grad_proj: bfloat16 [16, 3, 589824], P('data')
- weight_proj: float32 [3, 589824], P(None, 'data')
- mom_proj: float32 [3, 589824], P(None, 'data')
- var_proj: float32 [3, 589824], P(None, 'data')
- grad_fc_in: bfloat16 [16, 3, 2359296], P('data')
- weight_fc_in: float32 [3, 2359296], P(None, 'data')
- mom_fc_in: float32 [3, 2359296], P(None, 'data')
- var_fc_in: float32 [3, 2359296], P(None, 'data')
- grad_fc_out: bfloat16 [16, 3, 2359296], P('data')
- weight_fc_out: float32 [3, 2359296], P(None, 'data')
- mom_fc_out: float32 [3, 2359296], P(None, 'data')
- var_fc_out: float32 [3, 2359296], P(None, 'data')
Outputs:
- output 1: bfloat16 [3, 1769472], replicated
- output 2: float32 [3, 1769472], P(None, 'data')
- output 3: float32 [3, 1769472], P(None, 'data')
- output 4: float32 [3, 1769472], P(None, 'data')
- output 5: bfloat16 [3, 589824], replicated
- output 6: float32 [3, 589824], P(None, 'data')
- output 7: float32 [3, 589824], P(None, 'data')
- output 8: float32 [3, 589824], P(None, 'data')
- output 9: bfloat16 [3, 2359296], replicated
- output 10: float32 [3, 2359296], P(None, 'data')
- output 11: float32 [3, 2359296], P(None, 'data')
- output 12: float32 [3, 2359296], P(None, 'data')
- output 13: bfloat16 [3, 2359296], replicated
- output 14: float32 [3, 2359296], P(None, 'data')
- output 15: float32 [3, 2359296], P(None, 'data')
- output 16: float32 [3, 2359296], P(None, 'data')
All inputs are finite; a program needn't handle non-finite values.
Results may differ from the reference program's by a relative error of at most 0.001.
Values are sent between devices in bfloat16 or wider.
A program may use at most 1 GiB of HBM per device.

```python
import jax
import jax.numpy as jnp

D = 768
FF = 3072
LAYERS = 3
DATA = 16
STEP = 10

LEARN_RATE = 0.1
BETA_ONE = 0.9
BETA_TWO = 0.999
EPSILON = 1e-6
WEIGHT_DECAY = 0.01
TENSOR_SHAPES = ((D, 3 * D), (D, D), (D, FF), (FF, D))
KIND_NAMES = ("qkv", "proj", "fc_in", "fc_out")


def draw_tensor(rng_key, fan_in, fan_out):
    size_flat = fan_in * fan_out
    sub_keys = jax.random.split(rng_key, 8)
    position = jnp.arange(size_flat, dtype=jnp.float32) / size_flat - 0.5
    sign_flip = 2.0 * jax.random.randint(sub_keys[0], (LAYERS, 1), 0, 2).astype(jnp.float32) - 1.0
    ramp_slope = sign_flip * jax.random.uniform(sub_keys[1], (LAYERS, 1), minval=1.0, maxval=2.0)
    weight_scale = fan_in ** -0.5 * jnp.exp(jax.random.uniform(sub_keys[2], (LAYERS, 1), minval=-1.0, maxval=1.0))
    grad_scale = 10.0 * jnp.exp(jax.random.uniform(sub_keys[3], (LAYERS, 1), minval=-1.0, maxval=1.0))
    weight = weight_scale * jnp.exp(ramp_slope * position) * jax.random.normal(sub_keys[4], (LAYERS, size_flat))
    local_grad = grad_scale * DATA ** 0.5 * jax.random.normal(sub_keys[5], (DATA, LAYERS, size_flat))
    first_mom = 0.05 * grad_scale * jax.random.normal(sub_keys[6], (LAYERS, size_flat))
    second_mom = 0.0005 * grad_scale * grad_scale * jax.random.uniform(sub_keys[7], (LAYERS, size_flat), minval=0.5, maxval=1.5)
    return local_grad.astype(jnp.bfloat16), weight, first_mom, second_mom


def setup_inputs(seed: int = 0) -> dict:
    root_key = jax.random.key(seed)
    arrays = {}
    for kind_pos in range(4):
        fan_in, fan_out = TENSOR_SHAPES[kind_pos]
        drawn_set = draw_tensor(jax.random.fold_in(root_key, kind_pos), fan_in, fan_out)
        arrays["grad_" + KIND_NAMES[kind_pos]] = drawn_set[0]
        arrays["weight_" + KIND_NAMES[kind_pos]] = drawn_set[1]
        arrays["mom_" + KIND_NAMES[kind_pos]] = drawn_set[2]
        arrays["var_" + KIND_NAMES[kind_pos]] = drawn_set[3]
    return arrays


def lamb_tensor(local_grad, weight, first_mom, second_mom):
    grad_mean = jnp.sum(local_grad, axis=0, dtype=jnp.float32) / local_grad.shape[0]
    new_first = BETA_ONE * first_mom + (1.0 - BETA_ONE) * grad_mean
    new_second = BETA_TWO * second_mom + (1.0 - BETA_TWO) * grad_mean * grad_mean
    direction = (new_first / (1.0 - BETA_ONE ** STEP)) / (jnp.sqrt(new_second / (1.0 - BETA_TWO ** STEP)) + EPSILON) + WEIGHT_DECAY * weight
    weight_norm = jnp.sqrt(jnp.sum(weight * weight, axis=1, keepdims=True))
    update_norm = jnp.sqrt(jnp.sum(direction * direction, axis=1, keepdims=True))
    new_weight = weight - LEARN_RATE * (weight_norm / update_norm) * direction
    return new_weight.astype(jnp.bfloat16), new_weight, new_first, new_second


def reference(grad_qkv, weight_qkv, mom_qkv, var_qkv, grad_proj, weight_proj, mom_proj, var_proj, grad_fc_in, weight_fc_in, mom_fc_in, var_fc_in, grad_fc_out, weight_fc_out, mom_fc_out, var_fc_out):
    copy_qkv, new_weight_qkv, new_mom_qkv, new_var_qkv = lamb_tensor(grad_qkv, weight_qkv, mom_qkv, var_qkv)
    copy_proj, new_weight_proj, new_mom_proj, new_var_proj = lamb_tensor(grad_proj, weight_proj, mom_proj, var_proj)
    copy_fc_in, new_weight_fc_in, new_mom_fc_in, new_var_fc_in = lamb_tensor(grad_fc_in, weight_fc_in, mom_fc_in, var_fc_in)
    copy_fc_out, new_weight_fc_out, new_mom_fc_out, new_var_fc_out = lamb_tensor(grad_fc_out, weight_fc_out, mom_fc_out, var_fc_out)
    return (copy_qkv, new_weight_qkv, new_mom_qkv, new_var_qkv, copy_proj, new_weight_proj, new_mom_proj, new_var_proj, copy_fc_in, new_weight_fc_in, new_mom_fc_in, new_var_fc_in, copy_fc_out, new_weight_fc_out, new_mom_fc_out, new_var_fc_out)
```

```python
import functools

import jax
import jax.numpy as jnp
from jax import lax
from jax.experimental import pallas as pl
from jax.experimental.pallas import tpu as pltpu
from jax.sharding import PartitionSpec as P


STEP = 10
LEARN_RATE = 0.1
BETA_ONE = 0.9
BETA_TWO = 0.999
EPSILON = 1e-6
WEIGHT_DECAY = 0.01

MESH = pl.DeviceIdType.MESH
CHUNK = 12288
INNER = 1024
ORDERS = ((0, 1, 2), (1, 2, 0), (2, 0, 1))


def direction_of(grad_mean, weight, first_mom, second_mom):
    new_first = BETA_ONE * first_mom + (1.0 - BETA_ONE) * grad_mean
    new_second = BETA_TWO * second_mom + (1.0 - BETA_TWO) * grad_mean * grad_mean
    direction = (new_first / (1.0 - BETA_ONE ** STEP)) / (jnp.sqrt(new_second / (1.0 - BETA_TWO ** STEP)) + EPSILON) + WEIGHT_DECAY * weight
    return new_first, new_second, direction


def reduce_kernel(width, g_ref, w_ref, m_ref, v_ref, mean_ref, ratio_ref,
                  own, peer, pair, send1, keep, recv1, recv2, recv3, mean, wv, mv, vv, acc, part, parts, ratio,
                  own_sem, peer_send, peer_recv, s1, r1, s2, r2, s3, r3, state_sem, mean_sem, part_send, part_recv, ratio_sem):
    chunks = width // CHUNK
    me = lax.axis_index("data")
    core = me % 2
    bits = ((me // 2) % 2, (me // 4) % 2, (me // 8) % 2)
    partner = me + 1 - 2 * core
    neighbour = tuple(me + (2 << d) * (1 - 2 * bits[d]) for d in range(3))

    def shard_start(rel, parity):
        owner = parity
        for d in range(3):
            bit = (rel >> d) & 1
            owner = owner + (2 << d) * (1 - bits[d] if bit else bits[d])
        return owner * width

    def columns(rel, parity, t):
        return pl.ds(pl.multiple_of(shard_start(rel, parity) + t * CHUNK, 128), CHUNK)

    def load_own(t, rel):
        return pltpu.make_async_copy(g_ref.at[:, columns(rel, core, t)], own.at[t, rel], own_sem.at[t])

    def give_peer(t, rel):
        return pltpu.make_async_remote_copy(
            src_ref=g_ref.at[:, columns(rel, 1 - core, t)], dst_ref=peer.at[t, rel],
            send_sem=peer_send.at[t], recv_sem=peer_recv.at[t], device_id=(partner,), device_id_type=MESH)

    def stage(src, dst, ssem, rsem, dim):
        return pltpu.make_async_remote_copy(src_ref=src, dst_ref=dst, send_sem=ssem, recv_sem=rsem,
                                            device_id=(neighbour[dim],), device_id_type=MESH)

    def local_loop(t, _):
        for rel in range(8):
            load_own(t, rel).start()
        return 0

    lax.fori_loop(0, chunks, local_loop, 0)
    states = [pltpu.make_async_copy(src, dst, state_sem.at[i]) for i, (src, dst) in enumerate(((w_ref, wv), (m_ref, mv), (v_ref, vv)))]
    for copy in states:
        copy.start()
    barrier = pltpu.get_barrier_semaphore()
    for k in range(1, 16):
        pl.semaphore_signal(barrier, inc=1, device_id=((me + k) % 16,), device_id_type=MESH)
    pl.semaphore_wait(barrier, 15)

    def peer_loop(t, _):
        for rel in range(8):
            give_peer(t, rel).start()
        return 0

    lax.fori_loop(0, chunks, peer_loop, 0)
    acc[...] = jnp.zeros_like(acc)
    for copy in states:
        copy.wait()

    def pair_stage(t):
        pltpu.make_async_copy(own.at[t], own.at[t], own_sem.at[t]).wait()
        pltpu.make_async_copy(peer.at[t], peer.at[t], peer_recv.at[t]).wait()
        for rel in range(8):
            def inner(i, _, rel=rel):
                cols = pl.ds(pl.multiple_of(i * INNER, INNER), INNER)
                pair[rel] = own[t, rel, :, cols].astype(jnp.float32) + peer[t, rel, :, cols].astype(jnp.float32)
                for row in range(3):
                    a, b, c = ((rel >> d) & 1 for d in ORDERS[row])
                    dst = send1 if a else keep
                    dst[t, row, 2 * b + c, :, cols] = pair[rel, row:row + 1, :]
                return 0

            lax.fori_loop(0, CHUNK // INNER, inner, 0)
        for row in range(3):
            stage(send1.at[t, row], recv1.at[t, row], s1.at[t], r1.at[t], ORDERS[row][0]).start()

    def add_stage(t, recv, rsem, count):
        pltpu.make_async_copy(recv.at[t], recv.at[t], rsem.at[t]).wait()

        def inner(i, _):
            cols = pl.ds(pl.multiple_of(i * INNER, INNER), INNER)
            for row in range(3):
                for k in range(count):
                    keep[t, row, k, :, cols] = keep[t, row, k, :, cols] + recv[t, row, k, :, cols]
            return 0

        lax.fori_loop(0, CHUNK // INNER, inner, 0)

    def mean_copy(t):
        cols = pl.ds(pl.multiple_of(t * CHUNK, CHUNK), CHUNK)
        return pltpu.make_async_copy(mean.at[t], mean_ref.at[:, cols], mean_sem.at[t])

    def last_stage(t):
        pltpu.make_async_copy(recv3.at[t], recv3.at[t], r3.at[t]).wait()

        def inner(i, _):
            cols = pl.ds(pl.multiple_of(i * INNER, INNER), INNER)
            state_cols = pl.ds(pl.multiple_of(t * CHUNK + i * INNER, INNER), INNER)
            for row in range(3):
                total = (keep[t, row, 0, :, cols] + recv3[t, row, 0, :, cols]) / 16
                mean[t, row:row + 1, cols] = total
                weight = wv[row:row + 1, state_cols]
                direction = direction_of(total, weight, mv[row:row + 1, state_cols], vv[row:row + 1, state_cols])[2]
                acc[row] += weight * weight
                acc[3 + row] += direction * direction
            return 0

        lax.fori_loop(0, CHUNK // INNER, inner, 0)
        mean_copy(t).start()

    def step(t, _):
        @pl.when(t < chunks)
        def _():
            pair_stage(t)

        @pl.when((t >= 1) & (t < chunks + 1))
        def _():
            u = t - 1
            add_stage(u, recv1, r1, 4)
            for row in range(3):
                stage(keep.at[u, row, pl.ds(2, 2)], recv2.at[u, row], s2.at[u], r2.at[u], ORDERS[row][1]).start()

        @pl.when((t >= 2) & (t < chunks + 2))
        def _():
            u = t - 2
            add_stage(u, recv2, r2, 2)
            for row in range(3):
                stage(keep.at[u, row, pl.ds(1, 1)], recv3.at[u, row], s3.at[u], r3.at[u], ORDERS[row][2]).start()

        @pl.when(t >= 3)
        def _():
            last_stage(t - 3)

        return 0

    lax.fori_loop(0, chunks + 3, step, 0)

    for j in range(6):
        part[j:j + 1, :] = jnp.broadcast_to(jnp.sum(acc[j], axis=1, keepdims=True), (1, 128))
    for j in range(6, 8):
        part[j:j + 1, :] = jnp.zeros((1, 128), jnp.float32)
    parts[me] = part[...]
    shares = [pltpu.make_async_remote_copy(src_ref=part, dst_ref=parts.at[me], send_sem=part_send.at[k], recv_sem=part_recv.at[k],
                                           device_id=((me + k + 1) % 16,), device_id_type=MESH) for k in range(15)]
    for copy in shares:
        copy.start()

    def drain(t, _):
        pltpu.make_async_copy(peer.at[t], peer.at[t], peer_send.at[t]).wait()
        pltpu.make_async_copy(send1.at[t], send1.at[t], s1.at[t]).wait()
        pltpu.make_async_copy(recv2.at[t], recv2.at[t], s2.at[t]).wait()
        pltpu.make_async_copy(recv3.at[t], recv3.at[t], s3.at[t]).wait()
        mean_copy(t).wait()
        return 0

    lax.fori_loop(0, chunks, drain, 0)
    for copy in shares:
        copy.wait()
    total = parts[0]
    for i in range(1, 16):
        total = total + parts[i]
    norms = jnp.sqrt(total)
    ratio[...] = norms[0:3, :] / norms[3:6, :]
    copy = pltpu.make_async_copy(ratio, ratio_ref, ratio_sem)
    copy.start()
    copy.wait()


def reduce_and_norms(local_grad, weight, first_mom, second_mom, number):
    layers, width = weight.shape
    chunks = width // CHUNK
    f32, bf16 = jnp.float32, jnp.bfloat16
    dma = pltpu.SemaphoreType.DMA
    any_space = pl.BlockSpec(memory_space=pl.ANY)
    return pl.pallas_call(
        functools.partial(reduce_kernel, width),
        out_shape=(jax.ShapeDtypeStruct((layers, width), f32), jax.ShapeDtypeStruct((layers, 128), f32)),
        in_specs=[any_space] * 4,
        out_specs=(any_space, any_space),
        scratch_shapes=[
            pltpu.VMEM((chunks, 8, 3, CHUNK), bf16), pltpu.VMEM((chunks, 8, 3, CHUNK), bf16), pltpu.VMEM((8, 3, INNER), f32),
            pltpu.VMEM((chunks, 3, 4, 1, CHUNK), f32), pltpu.VMEM((chunks, 3, 4, 1, CHUNK), f32),
            pltpu.VMEM((chunks, 3, 4, 1, CHUNK), f32), pltpu.VMEM((chunks, 3, 2, 1, CHUNK), f32), pltpu.VMEM((chunks, 3, 1, 1, CHUNK), f32),
            pltpu.VMEM((chunks, 3, CHUNK), f32),
            pltpu.VMEM((3, width), f32), pltpu.VMEM((3, width), f32), pltpu.VMEM((3, width), f32),
            pltpu.VMEM((6, 1, INNER), f32), pltpu.VMEM((8, 128), f32), pltpu.VMEM((16, 8, 128), f32), pltpu.VMEM((3, 128), f32),
            dma((chunks,)), dma((chunks,)), dma((chunks,)),
            dma((chunks,)), dma((chunks,)), dma((chunks,)), dma((chunks,)), dma((chunks,)), dma((chunks,)),
            dma((3,)), dma((chunks,)), dma((15,)), dma((15,)), dma,
        ],
        compiler_params=pltpu.CompilerParams(collective_id=number, has_side_effects=True, vmem_limit_bytes=67043328),
        cost_estimate=pl.CostEstimate(flops=int(width * 2e6), bytes_accessed=width * 3 * 16 * 2, transcendentals=0),
    )(local_grad, weight, first_mom, second_mom)


def solution(mesh):
    grad_spec = P("data", None, None)
    shard_spec = P(None, "data")
    full_spec = P(None, None)

    def device_step(*blocks):
        results = [None] * 16
        last = None
        for number, kind in enumerate((2, 3, 0, 1)):
            local_grad, weight, first_mom, second_mom = blocks[4 * kind:4 * kind + 4]
            grad = local_grad.reshape(local_grad.shape[1:])
            if last is not None:
                grad = lax.optimization_barrier((grad, last))[0]
            mean, ratio = reduce_and_norms(grad, weight, first_mom, second_mom, number)
            new_first, new_second, direction = direction_of(mean, weight, first_mom, second_mom)
            new_weight = weight - LEARN_RATE * ratio[:, :1] * direction
            rounded = new_weight.astype(jnp.bfloat16)
            last = rounded
            replica = lax.all_gather(rounded, "data", axis=1, tiled=True)
            results[4 * kind:4 * kind + 4] = [replica, new_weight, new_first, new_second]
        return tuple(results)

    return jax.shard_map(device_step, mesh=mesh, in_specs=(grad_spec, shard_spec, shard_spec, shard_spec) * 4, out_specs=(full_spec, shard_spec, shard_spec, shard_spec) * 4, check_vma=False)
```

```python
import functools

import jax
import jax.numpy as jnp
from jax import lax
from jax.experimental import pallas as pl
from jax.experimental.pallas import tpu as pltpu
from jax.sharding import PartitionSpec as P

STEP = 10
LEARN_RATE = 0.1
BETA_ONE = 0.9
BETA_TWO = 0.999
EPSILON = 1e-6
WEIGHT_DECAY = 0.01

MESH = pl.DeviceIdType.MESH
CHUNK = 12288
INNER = 1024
PACKED = CHUNK * 3 // 4
THIRD = PACKED // 3
SLOTS = 4
LEAD = 2
KINDS = (2, 3, 0, 1)
COUNTS = (12, 12, 9, 3)
STARTS = (0, 12, 24, 33)
TOTAL = 36
ROOM = 39
PACK_AT = 16
ORDERS = ((0, 1, 2), (1, 2, 0), (2, 0, 1))


def place(chunk):
    return chunk + jnp.where(chunk >= STARTS[2], ROOM - TOTAL, 0)


def kind_of(chunk):
    return sum(jnp.where(chunk >= start, 1, 0) for start in STARTS[1:])


def step_kernel(*refs):
    states, refs = refs[:16], refs[16:]
    (gathered, out_w, out_m, out_v,
     own, peer, pair, send1, keep, recv1, recv2, recv3, wv, mv, vv, uv, acc, part, parts, ratio, quad, packed,
     own_sem, peer_send, peer_recv, s1, r1, s2, r2, s3, r3, state_sem, out_sem, part_send, part_recv,
     a1s, a2s, a3s, a1r, a2r, a3r, self_sem, mate_send, mate_recv) = refs
    me = lax.axis_index("data")
    core = me % 2
    bits = ((me // 2) % 2, (me // 4) % 2, (me // 8) % 2)
    partner = me + 1 - 2 * core
    neighbour = tuple(me + (2 << d) * (1 - 2 * bits[d]) for d in range(3))

    def owner(rel, parity):
        index = parity
        for d in range(3):
            index = index + (2 << d) * (1 - bits[d] if (rel >> d) & 1 else bits[d])
        return index

    def remote(src, dst, ssem, rsem, device):
        return pltpu.make_async_remote_copy(src_ref=src, dst_ref=dst, send_sem=ssem, recv_sem=rsem,
                                            device_id=(device,), device_id_type=MESH)

    def wait_for(ref, sem):
        pltpu.make_async_copy(ref, ref, sem).wait()

    def slot_of(chunk):
        return lax.rem(chunk, SLOTS)

    def for_kind(chunk, body):
        for kind in range(4):
            @pl.when((chunk >= STARTS[kind]) & (chunk < STARTS[kind] + COUNTS[kind]))
            def _(kind=kind):
                body(kind, chunk - STARTS[kind])

    def load_own(chunk):
        def body(kind, local):
            width = COUNTS[kind] * CHUNK
            slot = slot_of(chunk)
            for rel in range(8):
                cols = pl.ds(pl.multiple_of(owner(rel, core) * width + local * CHUNK, 128), CHUNK)
                pltpu.make_async_copy(states[4 * kind].at[:, cols], own.at[slot, rel], own_sem.at[slot]).start()
        for_kind(chunk, body)

    def give_peer(chunk):
        def body(kind, local):
            width = COUNTS[kind] * CHUNK
            slot = slot_of(chunk)
            for rel in range(8):
                cols = pl.ds(pl.multiple_of(owner(rel, 1 - core) * width + local * CHUNK, 128), CHUNK)
                remote(states[4 * kind].at[:, cols], peer.at[slot, rel], peer_send.at[slot], peer_recv.at[slot], partner).start()
        for_kind(chunk, body)

    def pair_stage(chunk):
        slot = slot_of(chunk)
        wait_for(own.at[slot], own_sem.at[slot])
        wait_for(peer.at[slot], peer_recv.at[slot])

        @pl.when(chunk >= SLOTS)
        def _():
            wait_for(send1.at[slot], s1.at[slot])
            wait_for(recv2.at[slot], s2.at[slot])
            wait_for(recv3.at[slot], s3.at[slot])

        for rel in range(8):
            def inner(i, _, rel=rel):
                cols = pl.ds(pl.multiple_of(i * INNER, INNER), INNER)
                pair[rel] = own[slot, rel, :, cols].astype(jnp.float32) + peer[slot, rel, :, cols].astype(jnp.float32)
                for row in range(3):
                    a, b, c = ((rel >> d) & 1 for d in ORDERS[row])
                    dst = send1 if a else keep
                    dst[slot, row, 2 * b + c, :, cols] = pair[rel, row:row + 1, :]
                return 0
            lax.fori_loop(0, CHUNK // INNER, inner, 0)
        for row in range(3):
            remote(send1.at[slot, row], recv1.at[slot, row], s1.at[slot], r1.at[slot], neighbour[ORDERS[row][0]]).start()

    def prefetch(chunk):
        @pl.when(chunk >= SLOTS)
        def _():
            wait_for(peer.at[slot_of(chunk)], peer_send.at[slot_of(chunk)])
        load_own(chunk)
        give_peer(chunk)

    def add_stage(slot, recv, rsem, count):
        wait_for(recv.at[slot], rsem.at[slot])

        def inner(i, _):
            cols = pl.ds(pl.multiple_of(i * INNER, INNER), INNER)
            for row in range(3):
                for k in range(count):
                    keep[slot, row, k, :, cols] = keep[slot, row, k, :, cols] + recv[slot, row, k, :, cols]
            return 0
        lax.fori_loop(0, CHUNK // INNER, inner, 0)

    def second_stage(chunk):
        slot = slot_of(chunk)
        add_stage(slot, recv1, r1, 4)
        for row in range(3):
            remote(keep.at[slot, row, pl.ds(2, 2)], recv2.at[slot, row], s2.at[slot], r2.at[slot], neighbour[ORDERS[row][1]]).start()

    def third_stage(chunk):
        slot = slot_of(chunk)
        add_stage(slot, recv2, r2, 2)
        for row in range(3):
            remote(keep.at[slot, row, pl.ds(1, 1)], recv3.at[slot, row], s3.at[slot], r3.at[slot], neighbour[ORDERS[row][2]]).start()

    def last_stage(chunk):
        slot = slot_of(chunk)
        kind = kind_of(chunk)
        wait_for(recv3.at[slot], r3.at[slot])

        def inner(i, _):
            cols = pl.ds(pl.multiple_of(i * INNER, INNER), INNER)
            for row in range(3):
                line = slice(row, row + 1)
                mean = (keep[slot, row, 0, :, cols] + recv3[slot, row, 0, :, cols]) / 16
                weight = wv[chunk, line, cols]
                new_first = BETA_ONE * mv[chunk, line, cols] + (1.0 - BETA_ONE) * mean
                new_second = BETA_TWO * vv[chunk, line, cols] + (1.0 - BETA_TWO) * mean * mean
                direction = (new_first / (1.0 - BETA_ONE ** STEP)) / (jnp.sqrt(new_second / (1.0 - BETA_TWO ** STEP)) + EPSILON) + WEIGHT_DECAY * weight
                mv[chunk, line, cols] = new_first
                vv[chunk, line, cols] = new_second
                uv[chunk, row, :, cols] = direction
                acc[kind, row] += weight * weight
                acc[kind, 3 + row] += direction * direction
            return 0
        lax.fori_loop(0, CHUNK // INNER, inner, 0)

    def send_norms(kind):
        for j in range(6):
            part[kind, j:j + 1, :] = jnp.broadcast_to(jnp.sum(acc[kind, j], axis=1, keepdims=True), (1, 128))
        for j in range(6, 8):
            part[kind, j:j + 1, :] = jnp.zeros((1, 128), jnp.float32)
        parts[kind, me] = part[kind]
        for k in range(1, 16):
            remote(part.at[kind], parts.at[kind, me], part_send.at[kind], part_recv.at[kind], (me + k) % 16).start()

    def take_norms(kind):
        wait_for(parts.at[kind, pl.ds(0, 15)], part_recv.at[kind])
        total = parts[kind, 0]
        for i in range(1, 16):
            total = total + parts[kind, i]
        norms = jnp.sqrt(total)
        trust = norms[0:3, :] / norms[3:6, :]
        for row in range(3):
            for i in range(INNER // 128):
                ratio[kind, row, :, i * 128:(i + 1) * 128] = trust[row:row + 1, :]

    def pack(chunk):
        kind = kind_of(chunk)

        def update(i, _):
            cols = pl.ds(pl.multiple_of(i * INNER, INNER), INNER)
            for row in range(3):
                line = slice(row, row + 1)
                wv[chunk, line, cols] = wv[chunk, line, cols] - LEARN_RATE * ratio[kind, row] * uv[chunk, row, :, cols]
            return 0
        lax.fori_loop(0, CHUNK // INNER, update, 0)
        for row in range(3):
            def fold(i, _, row=row):
                cols = pl.ds(pl.multiple_of(row * THIRD + i * INNER, INNER), INNER)
                tail = pl.ds(pl.multiple_of(PACKED + i * INNER, INNER), INNER)
                quad[0:3, :] = wv[chunk, :, cols]
                quad[3:4, :] = wv[chunk, row:row + 1, tail]
                packed[chunk, :, cols] = quad[...].astype(jnp.bfloat16)
                return 0
            lax.fori_loop(0, THIRD // INNER, fold, 0)

    def thirds(k):
        return pl.ds(k * THIRD, THIRD)

    def offset(*dims):
        return sum(1 << d for d in dims)

    def piece(rel, chunk, k):
        return gathered.at[owner(rel, core), place(chunk), :, thirds(k)]

    def to_partner(rel, chunk, k):
        remote(piece(rel, chunk, k), piece(rel, chunk, k), mate_send, mate_recv, partner).start()

    def gather_one(chunk):
        slot = slot_of(chunk)
        for k in range(3):
            remote(packed.at[chunk, :, thirds(k)], piece(0, chunk, k), a1s, a1r.at[slot], neighbour[ORDERS[k][0]]).start()
        mine = gathered.at[me, place(chunk)]
        remote(packed.at[chunk], mine, mate_send, mate_recv, partner).start()
        pltpu.make_async_copy(packed.at[chunk], mine, self_sem).start()
        for src, dst in ((wv, out_w), (mv, out_m), (vv, out_v)):
            pltpu.make_async_copy(src.at[chunk], dst.at[chunk], out_sem).start()

    def gather_two(chunk):
        slot = slot_of(chunk)
        wait_for(packed.at[0], a1r.at[slot])
        for k in range(3):
            a, b, c = ORDERS[k]
            remote(packed.at[chunk, :, thirds(k)], piece(0, chunk, k), a2s, a2r.at[slot], neighbour[b]).start()
            remote(piece(offset(a), chunk, k), piece(offset(a), chunk, k), a2s, a2r.at[slot], neighbour[b]).start()
        for k in range(3):
            to_partner(offset(ORDERS[k][0]), chunk, k)

    def gather_three(chunk):
        slot = slot_of(chunk)
        wait_for(packed.at[pl.ds(0, 2)], a2r.at[slot])
        for k in range(3):
            a, b, c = ORDERS[k]
            remote(packed.at[chunk, :, thirds(k)], piece(0, chunk, k), a3s, a3r.at[slot], neighbour[c]).start()
            for rel in (offset(a), offset(b), offset(a, b)):
                remote(piece(rel, chunk, k), piece(rel, chunk, k), a3s, a3r.at[slot], neighbour[c]).start()
        for k in range(3):
            a, b, c = ORDERS[k]
            to_partner(offset(b), chunk, k)
            to_partner(offset(a, b), chunk, k)

    def gather_four(chunk):
        wait_for(packed.at[pl.ds(0, 4)], a3r.at[slot_of(chunk)])
        for k in range(3):
            a, b, c = ORDERS[k]
            for rel in (offset(c), offset(a, c), offset(b, c), offset(a, b, c)):
                to_partner(rel, chunk, k)

    def at_chunk(chunk, body):
        @pl.when((chunk >= 0) & (chunk < TOTAL))
        def _():
            body(chunk)

    load_own(jnp.int32(0))
    load_own(jnp.int32(1))
    barrier = pltpu.get_barrier_semaphore()
    for k in range(1, 16):
        pl.semaphore_signal(barrier, inc=1, device_id=((me + k) % 16,), device_id_type=MESH)
    pl.semaphore_wait(barrier, 15)
    give_peer(jnp.int32(0))
    give_peer(jnp.int32(1))
    for kind in range(4):
        def load_states(i, _, kind=kind):
            cols = pl.ds(pl.multiple_of(i * CHUNK, CHUNK), CHUNK)
            for j, dst in enumerate((wv, mv, vv)):
                pltpu.make_async_copy(states[4 * kind + 1 + j].at[:, cols], dst.at[STARTS[kind] + i], state_sem.at[j]).start()
            return 0
        lax.fori_loop(0, COUNTS[kind], load_states, 0)
    acc[...] = jnp.zeros_like(acc)

    def step(s, _):
        at_chunk(s, pair_stage)
        @pl.when(s + LEAD < TOTAL)
        def _():
            prefetch(s + LEAD)
        at_chunk(s - 1, second_stage)
        at_chunk(s - 2, third_stage)

        @pl.when(s == 3)
        def _():
            for j, dst in enumerate((wv, mv, vv)):
                wait_for(dst, state_sem.at[j])
        at_chunk(s - 3, last_stage)
        for kind in range(4):
            @pl.when(s == STARTS[kind] + COUNTS[kind] + 2)
            def _(kind=kind):
                send_norms(kind)

            @pl.when(s == PACK_AT + STARTS[kind])
            def _(kind=kind):
                take_norms(kind)
        at_chunk(s - PACK_AT - 1, gather_one)
        at_chunk(s - PACK_AT - 2, gather_two)
        at_chunk(s - PACK_AT - 3, gather_three)
        at_chunk(s - PACK_AT - 4, gather_four)
        at_chunk(s - PACK_AT, pack)
        return 0

    lax.fori_loop(0, TOTAL + PACK_AT + 5, step, 0)

    def drain(chunk, _):
        slot = slot_of(chunk)
        wait_for(peer.at[slot], peer_send.at[slot])
        wait_for(send1.at[slot], s1.at[slot])
        wait_for(recv2.at[slot], s2.at[slot])
        wait_for(recv3.at[slot], s3.at[slot])
        return 0

    lax.fori_loop(TOTAL - SLOTS, TOTAL, drain, 0)
    for kind in range(4):
        wait_for(parts.at[kind, pl.ds(0, 15)], part_send.at[kind])
    wait_for(packed, a1s)
    wait_for(packed, self_sem)
    for dst in (wv, mv, vv):
        wait_for(dst, out_sem)
    live = pl.ds(0, TOTAL)
    wait_for(gathered.at[pl.ds(0, 2), live], a2s)
    wait_for(gathered.at[pl.ds(0, 4), live], a3s)
    wait_for(gathered.at[pl.ds(0, 8), live], mate_send)
    wait_for(gathered.at[pl.ds(0, 8), live], mate_recv)


def unpack_kernel(count, x_ref, o_ref, rows):
    for i in range(count):
        def head(j, _, i=i):
            cols = pl.ds(pl.multiple_of(j * INNER, INNER), INNER)
            out_cols = pl.ds(pl.multiple_of(i * CHUNK + j * INNER, INNER), INNER)
            o_ref[:, out_cols] = x_ref[0, i, 0:3, cols]
            return 0
        lax.fori_loop(0, PACKED // INNER, head, 0)

        def tail(j, _, i=i):
            for row in range(3):
                cols = pl.ds(pl.multiple_of(row * THIRD + j * INNER, INNER), INNER)
                rows[row:row + 1, :] = x_ref[0, i, 3:4, cols].astype(jnp.float32)
            out_cols = pl.ds(pl.multiple_of(i * CHUNK + PACKED + j * INNER, INNER), INNER)
            o_ref[:, out_cols] = rows[...].astype(jnp.bfloat16)
            return 0
        lax.fori_loop(0, THIRD // INNER, tail, 0)


def unpack(gathered, slot):
    count = COUNTS[slot]
    first = STARTS[slot] + (ROOM - TOTAL if slot >= 2 else 0)
    return pl.pallas_call(
        functools.partial(unpack_kernel, count),
        grid=(16,),
        out_shape=jax.ShapeDtypeStruct((3, 16 * count * CHUNK), jnp.bfloat16),
        in_specs=[pl.BlockSpec((1, count, 4, PACKED), lambda d: (d, first // count, 0, 0))],
        out_specs=pl.BlockSpec((3, count * CHUNK), lambda d: (0, d)),
        scratch_shapes=[pltpu.VMEM((3, INNER), jnp.float32)],
        compiler_params=pltpu.CompilerParams(vmem_limit_bytes=32 << 20),
        name="unpack_%d" % slot,
    )(gathered)


def optimizer_step(blocks):
    f32, bf16 = jnp.float32, jnp.bfloat16
    dma = pltpu.SemaphoreType.DMA
    any_space = pl.BlockSpec(memory_space=pl.ANY)
    operands = []
    for kind in KINDS:
        grad, weight, first_mom, second_mom = blocks[4 * kind:4 * kind + 4]
        operands += [grad.reshape(grad.shape[1:]), weight, first_mom, second_mom]
    state = jax.ShapeDtypeStruct((TOTAL, 3, CHUNK), f32)
    return pl.pallas_call(
        step_kernel,
        out_shape=(jax.ShapeDtypeStruct((16, ROOM, 4, PACKED), bf16), state, state, state),
        in_specs=[any_space] * 16,
        out_specs=(any_space,) * 4,
        scratch_shapes=[
            pltpu.VMEM((SLOTS, 8, 3, CHUNK), bf16), pltpu.VMEM((SLOTS, 8, 3, CHUNK), bf16), pltpu.VMEM((8, 3, INNER), f32),
            pltpu.VMEM((SLOTS, 3, 4, 1, CHUNK), f32), pltpu.VMEM((SLOTS, 3, 4, 1, CHUNK), f32),
            pltpu.VMEM((SLOTS, 3, 4, 1, CHUNK), f32), pltpu.VMEM((SLOTS, 3, 2, 1, CHUNK), f32), pltpu.VMEM((SLOTS, 3, 1, 1, CHUNK), f32),
            pltpu.VMEM((TOTAL, 3, CHUNK), f32), pltpu.VMEM((TOTAL, 3, CHUNK), f32), pltpu.VMEM((TOTAL, 3, CHUNK), f32),
            pltpu.VMEM((TOTAL, 3, 1, CHUNK), f32),
            pltpu.VMEM((4, 6, 1, INNER), f32), pltpu.VMEM((4, 8, 128), f32), pltpu.VMEM((4, 16, 8, 128), f32), pltpu.VMEM((4, 3, 1, INNER), f32),
            pltpu.VMEM((4, INNER), f32), pltpu.VMEM((TOTAL, 4, PACKED), bf16),
            dma((SLOTS,)), dma((SLOTS,)), dma((SLOTS,)),
            dma((SLOTS,)), dma((SLOTS,)), dma((SLOTS,)), dma((SLOTS,)), dma((SLOTS,)), dma((SLOTS,)),
            dma((3,)), dma, dma((4,)), dma((4,)),
            dma, dma, dma, dma((SLOTS,)), dma((SLOTS,)), dma((SLOTS,)), dma, dma, dma,
        ],
        compiler_params=pltpu.CompilerParams(collective_id=0, has_side_effects=True, vmem_limit_bytes=67043328),
        name="lamb_step",
    )(*operands)


def solution(mesh):
    grad_spec = P("data", None, None)
    shard_spec = P(None, "data")
    full_spec = P(None, None)

    def device_step(*blocks):
        gathered, *new_states = optimizer_step(blocks)
        results = [None] * 16
        for slot, kind in enumerate(KINDS):
            rows = slice(STARTS[slot], STARTS[slot] + COUNTS[slot])
            width = COUNTS[slot] * CHUNK
            results[4 * kind] = unpack(gathered, slot)
            results[4 * kind + 1:4 * kind + 4] = [x[rows].transpose(1, 0, 2).reshape(3, width) for x in new_states]
        return tuple(results)

    return jax.shard_map(device_step, mesh=mesh, in_specs=(grad_spec, shard_spec, shard_spec, shard_spec) * 4, out_specs=(full_spec, shard_spec, shard_spec, shard_spec) * 4, check_vma=False)
```

```python
import functools

import jax
import jax.numpy as jnp
from jax import lax
from jax.experimental import pallas as pl
from jax.experimental.pallas import tpu as pltpu
from jax.sharding import PartitionSpec as P

STEP = 10
LEARN_RATE = 0.1
BETA_ONE = 0.9
BETA_TWO = 0.999
EPSILON = 1e-6
WEIGHT_DECAY = 0.01

MESH = pl.DeviceIdType.MESH
CHUNK = 12288
INNER = 1024
PACKED = CHUNK * 3 // 4
THIRD = PACKED // 3
SLOTS = 4
LEAD = 2
KINDS = (2, 3, 0, 1)
COUNTS = (12, 12, 9, 3)
STARTS = (0, 12, 24, 33)
TOTAL = 36
ROOM = 39
PACK_AT = 16
GROUP = 3
DEPTH = 24
STATE_AT = 40
ORDERS = ((0, 1, 2), (1, 2, 0), (2, 0, 1))


def place(chunk):
    return chunk + jnp.where(chunk >= STARTS[2], ROOM - TOTAL, 0)


def kind_of(chunk):
    return sum(jnp.where(chunk >= start, 1, 0) for start in STARTS[1:])


def step_kernel(*refs):
    states, refs = refs[:16], refs[16:]
    (gathered, out_w, out_m, out_v,
     own, peer, pair, send1, keep, recv1, recv2, recv3, wv, mv, vv, uv, acc, part, parts, ratio, quad, packed,
     own_sem, peer_send, peer_recv, s1, r1, s2, r2, s3, r3, state_sem, out_sem, part_send, part_recv,
     a1s, a2s, a3s, a1r, a2r, a3r, self_sem, mate_send, mate_recv) = refs
    me = lax.axis_index("data")
    core = me % 2
    bits = ((me // 2) % 2, (me // 4) % 2, (me // 8) % 2)
    partner = me + 1 - 2 * core
    neighbour = tuple(me + (2 << d) * (1 - 2 * bits[d]) for d in range(3))

    def owner(rel, parity):
        index = parity
        for d in range(3):
            index = index + (2 << d) * (1 - bits[d] if (rel >> d) & 1 else bits[d])
        return index

    def remote(src, dst, ssem, rsem, device):
        return pltpu.make_async_remote_copy(src_ref=src, dst_ref=dst, send_sem=ssem, recv_sem=rsem,
                                            device_id=(device,), device_id_type=MESH)

    def wait_for(ref, sem):
        pltpu.make_async_copy(ref, ref, sem).wait()

    def slot_of(chunk):
        return lax.rem(chunk, SLOTS)

    def for_kind(chunk, body):
        for kind in range(4):
            @pl.when((chunk >= STARTS[kind]) & (chunk < STARTS[kind] + COUNTS[kind]))
            def _(kind=kind):
                body(kind, chunk - STARTS[kind])

    def load_own(chunk):
        def body(kind, local):
            width = COUNTS[kind] * CHUNK
            slot = slot_of(chunk)
            for rel in range(8):
                cols = pl.ds(pl.multiple_of(owner(rel, core) * width + local * CHUNK, 128), CHUNK)
                pltpu.make_async_copy(states[4 * kind].at[:, cols], own.at[slot, rel], own_sem.at[slot]).start()
        for_kind(chunk, body)

    def give_peer(chunk):
        def body(kind, local):
            width = COUNTS[kind] * CHUNK
            slot = slot_of(chunk)
            for rel in range(8):
                cols = pl.ds(pl.multiple_of(owner(rel, 1 - core) * width + local * CHUNK, 128), CHUNK)
                remote(states[4 * kind].at[:, cols], peer.at[slot, rel], peer_send.at[slot], peer_recv.at[slot], partner).start()
        for_kind(chunk, body)

    def pair_stage(chunk):
        slot = slot_of(chunk)
        wait_for(own.at[slot], own_sem.at[slot])
        wait_for(peer.at[slot], peer_recv.at[slot])

        @pl.when(chunk >= SLOTS)
        def _():
            wait_for(send1.at[slot], s1.at[slot])
            wait_for(recv2.at[slot], s2.at[slot])
            wait_for(recv3.at[slot], s3.at[slot])

        for rel in range(8):
            def inner(i, _, rel=rel):
                cols = pl.ds(pl.multiple_of(i * INNER, INNER), INNER)
                pair[rel] = own[slot, rel, :, cols].astype(jnp.float32) + peer[slot, rel, :, cols].astype(jnp.float32)
                for row in range(3):
                    a, b, c = ((rel >> d) & 1 for d in ORDERS[row])
                    dst = send1 if a else keep
                    dst[slot, row, 2 * b + c, :, cols] = pair[rel, row:row + 1, :]
                return 0
            lax.fori_loop(0, CHUNK // INNER, inner, 0)
        for row in range(3):
            remote(send1.at[slot, row], recv1.at[slot, row], s1.at[slot], r1.at[slot], neighbour[ORDERS[row][0]]).start()

    def prefetch(chunk):
        @pl.when(chunk >= SLOTS)
        def _():
            wait_for(peer.at[slot_of(chunk)], peer_send.at[slot_of(chunk)])
        load_own(chunk)
        give_peer(chunk)

    def add_stage(slot, recv, rsem, count):
        wait_for(recv.at[slot], rsem.at[slot])

        def inner(i, _):
            cols = pl.ds(pl.multiple_of(i * INNER, INNER), INNER)
            for row in range(3):
                for k in range(count):
                    keep[slot, row, k, :, cols] = keep[slot, row, k, :, cols] + recv[slot, row, k, :, cols]
            return 0
        lax.fori_loop(0, CHUNK // INNER, inner, 0)

    def second_stage(chunk):
        slot = slot_of(chunk)
        add_stage(slot, recv1, r1, 4)
        for row in range(3):
            remote(keep.at[slot, row, pl.ds(2, 2)], recv2.at[slot, row], s2.at[slot], r2.at[slot], neighbour[ORDERS[row][1]]).start()

    def third_stage(chunk):
        slot = slot_of(chunk)
        add_stage(slot, recv2, r2, 2)
        for row in range(3):
            remote(keep.at[slot, row, pl.ds(1, 1)], recv3.at[slot, row], s3.at[slot], r3.at[slot], neighbour[ORDERS[row][2]]).start()

    def last_stage(chunk):
        slot = slot_of(chunk)
        kind = kind_of(chunk)
        wait_for(recv3.at[slot], r3.at[slot])

        def inner(i, _):
            cols = pl.ds(pl.multiple_of(i * INNER, INNER), INNER)
            for row in range(3):
                line = slice(row, row + 1)
                mean = (keep[slot, row, 0, :, cols] + recv3[slot, row, 0, :, cols]) / 16
                weight = wv[chunk, line, cols]
                new_first = BETA_ONE * mv[chunk, line, cols] + (1.0 - BETA_ONE) * mean
                new_second = BETA_TWO * vv[chunk, line, cols] + (1.0 - BETA_TWO) * mean * mean
                direction = (new_first / (1.0 - BETA_ONE ** STEP)) / (jnp.sqrt(new_second / (1.0 - BETA_TWO ** STEP)) + EPSILON) + WEIGHT_DECAY * weight
                mv[chunk, line, cols] = new_first
                vv[chunk, line, cols] = new_second
                uv[chunk, row, :, cols] = direction
                acc[kind, row] += weight * weight
                acc[kind, 3 + row] += direction * direction
            return 0
        lax.fori_loop(0, CHUNK // INNER, inner, 0)

    def send_norms(kind):
        for j in range(6):
            part[kind, j:j + 1, :] = jnp.broadcast_to(jnp.sum(acc[kind, j], axis=1, keepdims=True), (1, 128))
        for j in range(6, 8):
            part[kind, j:j + 1, :] = jnp.zeros((1, 128), jnp.float32)
        parts[kind, me] = part[kind]
        for k in range(1, 16):
            remote(part.at[kind], parts.at[kind, me], part_send.at[kind], part_recv.at[kind], (me + k) % 16).start()

    def take_norms(kind):
        wait_for(parts.at[kind, pl.ds(0, 15)], part_recv.at[kind])
        total = parts[kind, 0]
        for i in range(1, 16):
            total = total + parts[kind, i]
        norms = jnp.sqrt(total)
        trust = norms[0:3, :] / norms[3:6, :]
        for row in range(3):
            for i in range(INNER // 128):
                ratio[kind, row, :, i * 128:(i + 1) * 128] = trust[row:row + 1, :]

    def pack(chunk):
        kind = kind_of(chunk)

        def update(i, _):
            cols = pl.ds(pl.multiple_of(i * INNER, INNER), INNER)
            for row in range(3):
                line = slice(row, row + 1)
                wv[chunk, line, cols] = wv[chunk, line, cols] - LEARN_RATE * ratio[kind, row] * uv[chunk, row, :, cols]
            return 0
        lax.fori_loop(0, CHUNK // INNER, update, 0)
        for row in range(3):
            def fold(i, _, row=row):
                cols = pl.ds(pl.multiple_of(row * THIRD + i * INNER, INNER), INNER)
                tail = pl.ds(pl.multiple_of(PACKED + i * INNER, INNER), INNER)
                quad[0:3, :] = wv[chunk, :, cols]
                quad[3:4, :] = wv[chunk, row:row + 1, tail]
                packed[chunk, :, cols] = quad[...].astype(jnp.bfloat16)
                return 0
            lax.fori_loop(0, THIRD // INNER, fold, 0)

    def thirds(k):
        return pl.ds(k * THIRD, THIRD)

    def offset(*dims):
        return sum(1 << d for d in dims)

    def piece(rel, chunk, k):
        return gathered.at[owner(rel, core), place(chunk), :, thirds(k)]

    def to_partner(rel, chunk, k):
        remote(piece(rel, chunk, k), piece(rel, chunk, k), mate_send, mate_recv, partner).start()

    def gather_one(chunk):
        slot = slot_of(chunk)
        for k in range(3):
            remote(packed.at[chunk, :, thirds(k)], piece(0, chunk, k), a1s, a1r.at[slot], neighbour[ORDERS[k][0]]).start()
        mine = gathered.at[me, place(chunk)]
        remote(packed.at[chunk], mine, mate_send, mate_recv, partner).start()
        pltpu.make_async_copy(packed.at[chunk], mine, self_sem).start()
        for src, dst in ((wv, out_w), (mv, out_m), (vv, out_v)):
            pltpu.make_async_copy(src.at[chunk], dst.at[chunk], out_sem).start()

    def gather_two(chunk):
        slot = slot_of(chunk)
        wait_for(packed.at[0], a1r.at[slot])
        for k in range(3):
            a, b, c = ORDERS[k]
            remote(packed.at[chunk, :, thirds(k)], piece(0, chunk, k), a2s, a2r.at[slot], neighbour[b]).start()
            remote(piece(offset(a), chunk, k), piece(offset(a), chunk, k), a2s, a2r.at[slot], neighbour[b]).start()
        for k in range(3):
            to_partner(offset(ORDERS[k][0]), chunk, k)

    def gather_three(chunk):
        slot = slot_of(chunk)
        wait_for(packed.at[pl.ds(0, 2)], a2r.at[slot])
        for k in range(3):
            a, b, c = ORDERS[k]
            remote(packed.at[chunk, :, thirds(k)], piece(0, chunk, k), a3s, a3r.at[slot], neighbour[c]).start()
            for rel in (offset(a), offset(b), offset(a, b)):
                remote(piece(rel, chunk, k), piece(rel, chunk, k), a3s, a3r.at[slot], neighbour[c]).start()
        for k in range(3):
            a, b, c = ORDERS[k]
            to_partner(offset(b), chunk, k)
            to_partner(offset(a, b), chunk, k)

    def gather_four(chunk):
        wait_for(packed.at[pl.ds(0, 4)], a3r.at[slot_of(chunk)])
        for k in range(3):
            a, b, c = ORDERS[k]
            for rel in (offset(c), offset(a, c), offset(b, c), offset(a, b, c)):
                to_partner(rel, chunk, k)

    def at_chunk(chunk, body):
        @pl.when((chunk >= 0) & (chunk < TOTAL))
        def _():
            body(chunk)

    load_own(jnp.int32(0))
    load_own(jnp.int32(1))
    barrier = pltpu.get_barrier_semaphore()
    for k in range(1, 16):
        pl.semaphore_signal(barrier, inc=1, device_id=((me + k) % 16,), device_id_type=MESH)
    pl.semaphore_wait(barrier, 15)
    give_peer(jnp.int32(0))
    give_peer(jnp.int32(1))
    for kind in range(4):
        def load_states(i, _, kind=kind):
            cols = pl.ds(pl.multiple_of(i * CHUNK, CHUNK), CHUNK)
            for j, dst in enumerate((wv, mv, vv)):
                pltpu.make_async_copy(states[4 * kind + 1 + j].at[:, cols], dst.at[STARTS[kind] + i], state_sem.at[j]).start()
            return 0
        lax.fori_loop(0, COUNTS[kind], load_states, 0)
    acc[...] = jnp.zeros_like(acc)

    def step(s, _):
        at_chunk(s, pair_stage)
        @pl.when(s + LEAD < TOTAL)
        def _():
            prefetch(s + LEAD)
        at_chunk(s - 1, second_stage)
        at_chunk(s - 2, third_stage)

        @pl.when(s == 3)
        def _():
            for j, dst in enumerate((wv, mv, vv)):
                wait_for(dst, state_sem.at[j])
        at_chunk(s - 3, last_stage)
        for kind in range(4):
            @pl.when(s == STARTS[kind] + COUNTS[kind] + 2)
            def _(kind=kind):
                send_norms(kind)

            @pl.when(s == PACK_AT + STARTS[kind])
            def _(kind=kind):
                take_norms(kind)
        at_chunk(s - PACK_AT - 1, gather_one)
        at_chunk(s - PACK_AT - 2, gather_two)
        at_chunk(s - PACK_AT - 3, gather_three)
        at_chunk(s - PACK_AT - 4, gather_four)
        at_chunk(s - PACK_AT, pack)
        return 0

    lax.fori_loop(0, TOTAL + PACK_AT + 5, step, 0)

    def drain(chunk, _):
        slot = slot_of(chunk)
        wait_for(peer.at[slot], peer_send.at[slot])
        wait_for(send1.at[slot], s1.at[slot])
        wait_for(recv2.at[slot], s2.at[slot])
        wait_for(recv3.at[slot], s3.at[slot])
        return 0

    lax.fori_loop(TOTAL - SLOTS, TOTAL, drain, 0)
    for kind in range(4):
        wait_for(parts.at[kind, pl.ds(0, 15)], part_send.at[kind])
    wait_for(packed, a1s)
    wait_for(packed, self_sem)
    for dst in (wv, mv, vv):
        wait_for(dst, out_sem)
    live = pl.ds(0, TOTAL)
    wait_for(gathered.at[pl.ds(0, 2), live], a2s)
    wait_for(gathered.at[pl.ds(0, 4), live], a3s)
    wait_for(gathered.at[pl.ds(0, 8), live], mate_send)
    wait_for(gathered.at[pl.ds(0, 8), live], mate_recv)


def finish_kernel(gathered, in_w, in_m, in_v, *refs):
    outs, refs = refs[:16], refs[16:]
    packed, full, rows, wv, mv, vv, load_sem, store_sem, in_sem, out_sem = refs
    groups = TOTAL // GROUP

    def load(unit):
        slot = lax.rem(unit, DEPTH)
        first = (unit // 16) * GROUP
        pltpu.make_async_copy(gathered.at[unit % 16, pl.ds(place(first), GROUP)], packed.at[slot], load_sem.at[slot]).start()

    def store(unit):
        slot = lax.rem(unit, DEPTH)
        first = (unit // 16) * GROUP
        for kind in range(4):
            @pl.when((first >= STARTS[kind]) & (first < STARTS[kind] + COUNTS[kind]))
            def _(kind=kind):
                begin = (unit % 16) * (COUNTS[kind] * CHUNK) + (first - STARTS[kind]) * CHUNK
                cols = pl.ds(pl.multiple_of(begin, CHUNK), GROUP * CHUNK)
                pltpu.make_async_copy(full.at[slot], outs[4 * kind].at[:, cols], store_sem.at[slot]).start()

    def wait_for(ref, sem):
        pltpu.make_async_copy(ref, ref, sem).wait()

    def unpack(slot):
        def one(i, _):
            for j in range(3):
                cols = pl.ds(j * THIRD, THIRD)
                out_cols = pl.ds(pl.multiple_of(i * CHUNK + j * THIRD, THIRD), THIRD)
                full[slot, :, out_cols] = packed[slot, i, 0:3, cols]
                rows[j:j + 1, :] = packed[slot, i, 3:4, cols].astype(jnp.float32)
            out_cols = pl.ds(pl.multiple_of(i * CHUNK + PACKED, THIRD), THIRD)
            full[slot, :, out_cols] = rows[...].astype(jnp.bfloat16)
            return 0
        lax.fori_loop(0, GROUP, one, 0)

    def fill(unit, _):
        load(unit)
        return 0

    lax.fori_loop(0, DEPTH, fill, 0)
    pairs = ((in_w, wv), (in_m, mv), (in_v, vv))
    for j, (src, dst) in enumerate(pairs):
        pltpu.make_async_copy(src, dst, in_sem.at[j]).start()

    def step(unit, _):
        slot = lax.rem(unit, DEPTH)
        wait_for(packed.at[slot], load_sem.at[slot])

        @pl.when(unit >= DEPTH)
        def _():
            wait_for(full.at[slot], store_sem.at[slot])
        unpack(slot)
        store(unit)

        @pl.when(unit + DEPTH < 16 * groups)
        def _():
            load(unit + DEPTH)

        for j, (_src, dst) in enumerate(pairs):
            @pl.when(unit == STATE_AT * (j + 1))
            def _(j=j, dst=dst):
                wait_for(dst, in_sem.at[j])
                for kind in range(4):
                    def put(i, _, kind=kind):
                        cols = pl.ds(pl.multiple_of(i * CHUNK, CHUNK), CHUNK)
                        pltpu.make_async_copy(dst.at[STARTS[kind] + i], outs[4 * kind + 1 + j].at[:, cols], out_sem.at[j]).start()
                        return 0
                    lax.fori_loop(0, COUNTS[kind], put, 0)
        return 0

    lax.fori_loop(0, 16 * groups, step, 0)

    def drain(slot, _):
        wait_for(full.at[slot], store_sem.at[slot])
        return 0

    lax.fori_loop(0, DEPTH, drain, 0)
    for j, (_src, dst) in enumerate(pairs):
        wait_for(dst, out_sem.at[j])


def finish(gathered, new_states):
    f32, bf16 = jnp.float32, jnp.bfloat16
    dma = pltpu.SemaphoreType.DMA
    any_space = pl.BlockSpec(memory_space=pl.ANY)
    shapes = []
    for count in COUNTS:
        shapes += [jax.ShapeDtypeStruct((3, 16 * count * CHUNK), bf16)] + [jax.ShapeDtypeStruct((3, count * CHUNK), f32)] * 3
    return pl.pallas_call(
        finish_kernel,
        out_shape=tuple(shapes),
        in_specs=[any_space] * 4,
        out_specs=(any_space,) * 16,
        scratch_shapes=[
            pltpu.VMEM((DEPTH, GROUP, 4, PACKED), bf16), pltpu.VMEM((DEPTH, 3, GROUP * CHUNK), bf16), pltpu.VMEM((3, THIRD), f32),
            pltpu.VMEM((TOTAL, 3, CHUNK), f32), pltpu.VMEM((TOTAL, 3, CHUNK), f32), pltpu.VMEM((TOTAL, 3, CHUNK), f32),
            dma((DEPTH,)), dma((DEPTH,)), dma((3,)), dma((3,)),
        ],
        compiler_params=pltpu.CompilerParams(vmem_limit_bytes=67043328),
        name="finish",
    )(gathered, *new_states)


def optimizer_step(blocks):
    f32, bf16 = jnp.float32, jnp.bfloat16
    dma = pltpu.SemaphoreType.DMA
    any_space = pl.BlockSpec(memory_space=pl.ANY)
    operands = []
    for kind in KINDS:
        grad, weight, first_mom, second_mom = blocks[4 * kind:4 * kind + 4]
        operands += [grad.reshape(grad.shape[1:]), weight, first_mom, second_mom]
    state = jax.ShapeDtypeStruct((TOTAL, 3, CHUNK), f32)
    return pl.pallas_call(
        step_kernel,
        out_shape=(jax.ShapeDtypeStruct((16, ROOM, 4, PACKED), bf16), state, state, state),
        in_specs=[any_space] * 16,
        out_specs=(any_space,) * 4,
        scratch_shapes=[
            pltpu.VMEM((SLOTS, 8, 3, CHUNK), bf16), pltpu.VMEM((SLOTS, 8, 3, CHUNK), bf16), pltpu.VMEM((8, 3, INNER), f32),
            pltpu.VMEM((SLOTS, 3, 4, 1, CHUNK), f32), pltpu.VMEM((SLOTS, 3, 4, 1, CHUNK), f32),
            pltpu.VMEM((SLOTS, 3, 4, 1, CHUNK), f32), pltpu.VMEM((SLOTS, 3, 2, 1, CHUNK), f32), pltpu.VMEM((SLOTS, 3, 1, 1, CHUNK), f32),
            pltpu.VMEM((TOTAL, 3, CHUNK), f32), pltpu.VMEM((TOTAL, 3, CHUNK), f32), pltpu.VMEM((TOTAL, 3, CHUNK), f32),
            pltpu.VMEM((TOTAL, 3, 1, CHUNK), f32),
            pltpu.VMEM((4, 6, 1, INNER), f32), pltpu.VMEM((4, 8, 128), f32), pltpu.VMEM((4, 16, 8, 128), f32), pltpu.VMEM((4, 3, 1, INNER), f32),
            pltpu.VMEM((4, INNER), f32), pltpu.VMEM((TOTAL, 4, PACKED), bf16),
            dma((SLOTS,)), dma((SLOTS,)), dma((SLOTS,)),
            dma((SLOTS,)), dma((SLOTS,)), dma((SLOTS,)), dma((SLOTS,)), dma((SLOTS,)), dma((SLOTS,)),
            dma((3,)), dma, dma((4,)), dma((4,)),
            dma, dma, dma, dma((SLOTS,)), dma((SLOTS,)), dma((SLOTS,)), dma, dma, dma,
        ],
        compiler_params=pltpu.CompilerParams(collective_id=0, has_side_effects=True, vmem_limit_bytes=67043328),
        name="lamb_step",
    )(*operands)


def solution(mesh):
    grad_spec = P("data", None, None)
    shard_spec = P(None, "data")
    full_spec = P(None, None)

    def device_step(*blocks):
        gathered, *new_states = optimizer_step(blocks)
        outs = finish(gathered, new_states)
        results = [None] * 16
        for slot, kind in enumerate(KINDS):
            results[4 * kind:4 * kind + 4] = outs[4 * slot:4 * slot + 4]
        return tuple(results)

    return jax.shard_map(device_step, mesh=mesh, in_specs=(grad_spec, shard_spec, shard_spec, shard_spec) * 4, out_specs=(full_spec, shard_spec, shard_spec, shard_spec) * 4, check_vma=False)
```

```python
import functools

import jax
import jax.numpy as jnp
from jax import lax
from jax.experimental import pallas as pl
from jax.experimental.pallas import tpu as pltpu
from jax.sharding import PartitionSpec as P


STEP = 10
LEARN_RATE = 0.1
BETA_ONE = 0.9
BETA_TWO = 0.999
EPSILON = 1e-6
WEIGHT_DECAY = 0.01

MESH = pl.DeviceIdType.MESH
CHUNK = 12288
INNER = 1024
PACKED = CHUNK * 3 // 4
THIRD = PACKED // 3
PART = CHUNK // 3
SLOTS = 4
LEAD = 2
KINDS = (2, 3, 0, 1)
COUNTS = (12, 12, 9, 3)
STARTS = (0, 12, 24, 33)
TOTAL = 36
MOVED = 15
STEP_VMEM = 28 << 20
LAST_VMEM = 13 << 20
FAR_VMEM = 6 << 20
PACK_AT = 17
GROUP = 3
DEPTH = 12
RING = 4
ORDERS = ((0, 1, 2), (1, 2, 0), (2, 0, 1))


def kind_of(chunk):
    return sum(jnp.where(chunk >= start, 1, 0) for start in STARTS[1:])


def step_kernel(*refs):
    states, refs = refs[:16], refs[16:]
    (gathered, near_0, near_1, near_2, mate, wv, mv, vv,
     own, peer, pair, send1, keep, recv1, recv2, recv3, uv, acc, part, parts, ratio, quad, packed,
     own_sem, peer_send, peer_recv, s1, r1, s2, r2, s3, r3, state_sem, part_send, part_recv,
     a1s, a2s, a3s, a1r, a2r, a3r, self_sem, mate_send, mate_recv, a2n, near_send, near_recv) = refs
    near = (near_0, near_1, near_2)
    me = lax.axis_index("data")
    core = me % 2
    bits = ((me // 2) % 2, (me // 4) % 2, (me // 8) % 2)
    partner = me + 1 - 2 * core
    neighbour = tuple(me + (2 << d) * (1 - 2 * bits[d]) for d in range(3))

    def owner(rel, parity):
        index = parity
        for d in range(3):
            index = index + (2 << d) * (1 - bits[d] if (rel >> d) & 1 else bits[d])
        return index

    def remote(src, dst, ssem, rsem, device):
        return pltpu.make_async_remote_copy(src_ref=src, dst_ref=dst, send_sem=ssem, recv_sem=rsem,
                                            device_id=(device,), device_id_type=MESH)

    def wait_for(ref, sem):
        pltpu.make_async_copy(ref, ref, sem).wait()

    def slot_of(chunk):
        return lax.rem(chunk, SLOTS)

    def for_kind(chunk, body):
        for kind in range(4):
            @pl.when((chunk >= STARTS[kind]) & (chunk < STARTS[kind] + COUNTS[kind]))
            def _(kind=kind):
                body(kind, chunk - STARTS[kind])

    def load_own(chunk):
        def body(kind, local):
            width = COUNTS[kind] * CHUNK
            slot = slot_of(chunk)
            for rel in range(8):
                cols = pl.ds(pl.multiple_of(owner(rel, core) * width + local * CHUNK, 128), CHUNK)
                pltpu.make_async_copy(states[4 * kind].at[:, cols], own.at[slot, rel], own_sem.at[slot]).start()

        for_kind(chunk, body)

    def give_peer(chunk):
        def body(kind, local):
            width = COUNTS[kind] * CHUNK
            slot = slot_of(chunk)
            for rel in range(8):
                cols = pl.ds(pl.multiple_of(owner(rel, 1 - core) * width + local * CHUNK, 128), CHUNK)
                remote(states[4 * kind].at[:, cols], peer.at[slot, rel], peer_send.at[slot], peer_recv.at[slot], partner).start()

        for_kind(chunk, body)

    def pair_stage(chunk):
        slot = slot_of(chunk)
        wait_for(own.at[slot], own_sem.at[slot])
        wait_for(peer.at[slot], peer_recv.at[slot])

        @pl.when(chunk >= SLOTS)
        def _():
            wait_for(send1.at[slot], s1.at[slot])
            wait_for(recv2.at[slot], s2.at[slot])
            wait_for(recv3.at[slot], s3.at[slot])

        for rel in range(8):
            def inner(i, _, rel=rel):
                cols = pl.ds(pl.multiple_of(i * INNER, INNER), INNER)
                pair[rel] = own[slot, rel, :, cols].astype(jnp.float32) + peer[slot, rel, :, cols].astype(jnp.float32)
                for row in range(3):
                    a, b, c = ((rel >> d) & 1 for d in ORDERS[row])
                    dst = send1 if a else keep
                    dst[slot, row, 2 * b + c, :, cols] = pair[rel, row:row + 1, :]
                return 0

            lax.fori_loop(0, CHUNK // INNER, inner, 0)
        for row in range(3):
            remote(send1.at[slot, row], recv1.at[slot, row], s1.at[slot], r1.at[slot], neighbour[ORDERS[row][0]]).start()

    def prefetch(chunk):
        @pl.when(chunk >= SLOTS)
        def _():
            wait_for(peer.at[slot_of(chunk)], peer_send.at[slot_of(chunk)])

        load_own(chunk)
        give_peer(chunk)

    def add_stage(slot, recv, rsem, count):
        wait_for(recv.at[slot], rsem.at[slot])

        def inner(i, _):
            cols = pl.ds(pl.multiple_of(i * INNER, INNER), INNER)
            for row in range(3):
                for k in range(count):
                    keep[slot, row, k, :, cols] = keep[slot, row, k, :, cols] + recv[slot, row, k, :, cols]
            return 0

        lax.fori_loop(0, CHUNK // INNER, inner, 0)

    def second_stage(chunk):
        slot = slot_of(chunk)
        add_stage(slot, recv1, r1, 4)
        for row in range(3):
            remote(keep.at[slot, row, pl.ds(2, 2)], recv2.at[slot, row], s2.at[slot], r2.at[slot], neighbour[ORDERS[row][1]]).start()

    def third_stage(chunk):
        slot = slot_of(chunk)
        add_stage(slot, recv2, r2, 2)
        for row in range(3):
            remote(keep.at[slot, row, pl.ds(1, 1)], recv3.at[slot, row], s3.at[slot], r3.at[slot], neighbour[ORDERS[row][2]]).start()

    def last_stage(chunk):
        slot = slot_of(chunk)
        kind = kind_of(chunk)
        wait_for(recv3.at[slot], r3.at[slot])

        def inner(i, _):
            cols = pl.ds(pl.multiple_of(i * INNER, INNER), INNER)
            for row in range(3):
                line = slice(row, row + 1)
                mean = (keep[slot, row, 0, :, cols] + recv3[slot, row, 0, :, cols]) / 16
                weight = wv[chunk, line, cols]
                new_first = BETA_ONE * mv[chunk, line, cols] + (1.0 - BETA_ONE) * mean
                new_second = BETA_TWO * vv[chunk, line, cols] + (1.0 - BETA_TWO) * mean * mean
                direction = (new_first / (1.0 - BETA_ONE ** STEP)) / (jnp.sqrt(new_second / (1.0 - BETA_TWO ** STEP)) + EPSILON) + WEIGHT_DECAY * weight
                mv[chunk, line, cols] = new_first
                vv[chunk, line, cols] = new_second
                uv[chunk, row, :, cols] = direction
                acc[kind, row] += weight * weight
                acc[kind, 3 + row] += direction * direction
            return 0

        lax.fori_loop(0, CHUNK // INNER, inner, 0)

    def send_norms(kind):
        for j in range(6):
            part[kind, j:j + 1, :] = jnp.broadcast_to(jnp.sum(acc[kind, j], axis=1, keepdims=True), (1, 128))
        for j in range(6, 8):
            part[kind, j:j + 1, :] = jnp.zeros((1, 128), jnp.float32)
        parts[kind, me] = part[kind]
        for k in range(1, 16):
            remote(part.at[kind], parts.at[kind, me], part_send.at[kind], part_recv.at[kind], (me + k) % 16).start()

    def take_norms(kind):
        wait_for(parts.at[kind, pl.ds(0, 15)], part_recv.at[kind])
        total = parts[kind, 0]
        for i in range(1, 16):
            total = total + parts[kind, i]
        norms = jnp.sqrt(total)
        trust = norms[0:3, :] / norms[3:6, :]
        for row in range(3):
            for i in range(INNER // 128):
                ratio[kind, row, :, i * 128:(i + 1) * 128] = trust[row:row + 1, :]

    def update(chunk):
        kind = kind_of(chunk)

        def inner(i, _):
            cols = pl.ds(pl.multiple_of(i * INNER, INNER), INNER)
            for row in range(3):
                line = slice(row, row + 1)
                wv[chunk, line, cols] = wv[chunk, line, cols] - LEARN_RATE * ratio[kind, row] * uv[chunk, row, :, cols]
            return 0

        lax.fori_loop(0, CHUNK // INNER, inner, 0)

    def pack(unit):
        begin = lax.rem(unit, GROUP) * PART
        for k in range(3):
            chunk = unit - lax.rem(unit, GROUP) + k
            for row in range(3):
                head = pl.ds(pl.multiple_of(begin + row * INNER, INNER), INNER)
                tail = pl.ds(pl.multiple_of(begin + THIRD, INNER), INNER)
                quad[row, 0:3, :] = wv[chunk, :, head]
                quad[row, 3:4, :] = wv[chunk, row:row + 1, tail]
                packed[unit, :, k * THIRD + row * INNER:k * THIRD + (row + 1) * INNER] = quad[row].astype(jnp.bfloat16)

    def thirds(k):
        return pl.ds(k * THIRD, THIRD)

    def offset(*dims):
        return sum(1 << d for d in dims)

    def piece(rel, chunk, k):
        return gathered.at[owner(rel, core), chunk - MOVED, :, thirds(k)]

    def to_partner(rel, chunk, k):
        remote(piece(rel, chunk, k), piece(rel, chunk, k), mate_send, mate_recv, partner).start()

    def near_to_partner(k, j, chunk):
        remote(near[k].at[j, chunk], mate.at[k, j, chunk], near_send, near_recv, partner).start()

    def gather_one(chunk):
        slot = slot_of(chunk)

        @pl.when(chunk < MOVED)
        def _():
            for k in range(3):
                mine = packed.at[chunk, :, thirds(k)]
                remote(mine, near[k].at[1, chunk], a1s, a1r.at[slot], neighbour[ORDERS[k][0]]).start()
                remote(mine, mate.at[k, 0, chunk], near_send, near_recv, partner).start()
                pltpu.make_async_copy(mine, near[k].at[0, chunk], self_sem).start()

        @pl.when(chunk >= MOVED)
        def _():
            for k in range(3):
                remote(packed.at[chunk, :, thirds(k)], piece(0, chunk, k), a1s, a1r.at[slot], neighbour[ORDERS[k][0]]).start()
            mine = gathered.at[me, chunk - MOVED]
            remote(packed.at[chunk], mine, mate_send, mate_recv, partner).start()
            pltpu.make_async_copy(packed.at[chunk], mine, self_sem).start()

    def gather_two(chunk):
        slot = slot_of(chunk)
        wait_for(packed.at[0], a1r.at[slot])

        @pl.when(chunk < MOVED)
        def _():
            for k in range(3):
                device = neighbour[ORDERS[k][1]]
                remote(packed.at[chunk, :, thirds(k)], near[k].at[2, chunk], a2n, a2r.at[slot], device).start()
                remote(near[k].at[1, chunk], near[k].at[3, chunk], a2n, a2r.at[slot], device).start()
            for k in range(3):
                near_to_partner(k, 1, chunk)

        @pl.when(chunk >= MOVED)
        def _():
            for k in range(3):
                a, b, _ = ORDERS[k]
                remote(packed.at[chunk, :, thirds(k)], piece(0, chunk, k), a2s, a2r.at[slot], neighbour[b]).start()
                remote(piece(offset(a), chunk, k), piece(offset(a), chunk, k), a2s, a2r.at[slot], neighbour[b]).start()
            for k in range(3):
                to_partner(offset(ORDERS[k][0]), chunk, k)

    def gather_three(chunk):
        slot = slot_of(chunk)
        wait_for(packed.at[pl.ds(0, 2)], a2r.at[slot])

        @pl.when(chunk < MOVED)
        def _():
            for k in range(3):
                near_to_partner(k, 2, chunk)
                near_to_partner(k, 3, chunk)

        @pl.when(chunk >= MOVED)
        def _():
            for k in range(3):
                a, b, c = ORDERS[k]
                remote(packed.at[chunk, :, thirds(k)], piece(0, chunk, k), a3s, a3r.at[slot], neighbour[c]).start()
                for rel in (offset(a), offset(b), offset(a, b)):
                    remote(piece(rel, chunk, k), piece(rel, chunk, k), a3s, a3r.at[slot], neighbour[c]).start()
            for k in range(3):
                a, b, c = ORDERS[k]
                to_partner(offset(b), chunk, k)
                to_partner(offset(a, b), chunk, k)

    def gather_four(chunk):
        @pl.when(chunk >= MOVED)
        def _():
            wait_for(packed.at[pl.ds(0, 4)], a3r.at[slot_of(chunk)])
            for k in range(3):
                a, b, c = ORDERS[k]
                for rel in (offset(c), offset(a, c), offset(b, c), offset(a, b, c)):
                    to_partner(rel, chunk, k)

    def at_chunk(chunk, body):
        @pl.when((chunk >= 0) & (chunk < TOTAL))
        def _():
            body(chunk)

    load_own(jnp.int32(0))
    load_own(jnp.int32(1))
    barrier = pltpu.get_barrier_semaphore()
    for k in range(1, 16):
        pl.semaphore_signal(barrier, inc=1, device_id=((me + k) % 16,), device_id_type=MESH)
    pl.semaphore_wait(barrier, 15)
    give_peer(jnp.int32(0))
    give_peer(jnp.int32(1))
    acc[...] = jnp.zeros_like(acc)

    def step(s, _):
        at_chunk(s, pair_stage)

        @pl.when(s + LEAD < TOTAL)
        def _():
            prefetch(s + LEAD)

        @pl.when(s == 0)
        def _():
            for kind in range(4):
                def load_states(i, _, kind=kind):
                    cols = pl.ds(pl.multiple_of(i * CHUNK, CHUNK), CHUNK)
                    for j, dst in enumerate((wv, mv, vv)):
                        pltpu.make_async_copy(states[4 * kind + 1 + j].at[:, cols], dst.at[STARTS[kind] + i], state_sem.at[j]).start()
                    return 0

                lax.fori_loop(0, COUNTS[kind], load_states, 0)

        at_chunk(s - 1, second_stage)
        at_chunk(s - 2, third_stage)

        @pl.when(s == 3)
        def _():
            for j, dst in enumerate((wv, mv, vv)):
                wait_for(dst, state_sem.at[j])

        at_chunk(s - 3, last_stage)
        for kind in range(4):
            @pl.when(s == STARTS[kind] + COUNTS[kind] + 2)
            def _(kind=kind):
                send_norms(kind)

            @pl.when(s == PACK_AT - 2 + STARTS[kind])
            def _(kind=kind):
                take_norms(kind)
        at_chunk(s - PACK_AT - 1, gather_one)
        at_chunk(s - PACK_AT - 2, gather_two)
        at_chunk(s - PACK_AT - 3, gather_three)
        at_chunk(s - PACK_AT - 4, gather_four)
        at_chunk(s - PACK_AT + 2, update)
        at_chunk(s - PACK_AT, pack)
        return 0

    lax.fori_loop(0, TOTAL + PACK_AT + 5, step, 0)

    def drain(chunk, _):
        slot = slot_of(chunk)
        wait_for(peer.at[slot], peer_send.at[slot])
        wait_for(send1.at[slot], s1.at[slot])
        wait_for(recv2.at[slot], s2.at[slot])
        wait_for(recv3.at[slot], s3.at[slot])
        return 0

    lax.fori_loop(TOTAL - SLOTS, TOTAL, drain, 0)
    for kind in range(4):
        wait_for(parts.at[kind, pl.ds(0, 15)], part_send.at[kind])
    wait_for(packed, a1s)
    wait_for(packed, self_sem)
    wait_for(gathered.at[pl.ds(0, 2)], a2s)
    wait_for(mate.at[:, pl.ds(0, 2)], a2n)
    wait_for(gathered.at[pl.ds(0, 4)], a3s)
    for sem in (mate_send, mate_recv):
        wait_for(gathered.at[pl.ds(0, 8)], sem)
    for sem in (near_send, near_recv):
        wait_for(mate, sem)


def wait_for(ref, sem):
    pltpu.make_async_copy(ref, ref, sem).wait()


def in_vmem(x):
    return pltpu.with_memory_space_constraint(x, pltpu.VMEM)


def unpack_part(src, dst, col, rows):
    dst[:, pl.ds(col, THIRD)] = src[0:3, :]
    for row in range(3):
        rows[row:row + 1, :] = src[3:4, row * INNER:(row + 1) * INNER].astype(jnp.float32)
    dst[:, pl.ds(col + THIRD, INNER)] = rows[...].astype(jnp.bfloat16)


class MovedRing:
    def __init__(self, sources, far, outs, buffers):
        self.sources, self.far, self.outs = sources, far, outs
        self.full, self.rows, self.store_sem = buffers
        self.groups = MOVED // GROUP
        self.steps = 4 * self.groups
        me = lax.axis_index("data")
        self.core = me % 2
        self.bits = ((me // 2) % 2, (me // 4) % 2, (me // 8) % 2)

    def store(self, step):
        slot = lax.rem(step, RING)
        j, group = step // self.groups, lax.rem(step, self.groups)
        for i, (_, k, other) in enumerate(self.sources):
            rel = [0, 0, 0]
            for d, bit in zip(ORDERS[k], (j % 2, j // 2, self.far)):
                rel[d] = bit
            shard = self.core + other - 2 * other * self.core
            for d in range(3):
                shard = shard + (2 << d) * (self.bits[d] + rel[d] - 2 * self.bits[d] * rel[d])
            for kind in range(2):
                @pl.when((group >= COUNTS[0] // GROUP) if kind else (group < COUNTS[0] // GROUP))
                def _(kind=kind, i=i, k=k, shard=shard):
                    begin = (shard * COUNTS[kind] + group * GROUP + k - STARTS[kind]) * CHUNK
                    pltpu.make_async_copy(self.full.at[slot, i], self.outs[kind].at[:, pl.ds(pl.multiple_of(begin, CHUNK), CHUNK)],
                                          self.store_sem.at[slot]).start()

    def run(self):
        def body(step, _):
            slot = lax.rem(step, RING)

            @pl.when(step >= RING)
            def _():
                wait_for(self.full.at[slot], self.store_sem.at[slot])

            j, first = step // self.groups, lax.rem(step, self.groups) * GROUP
            for i, (source, _, _) in enumerate(self.sources):
                for c in range(GROUP):
                    unpack_part(source.at[j, first + c], self.full.at[slot, i], c * PART, self.rows.at[c])
            self.store(step)
            return 0

        lax.fori_loop(0, self.steps, body, 0)

    def drain(self):
        for slot in range(RING):
            wait_for(self.full.at[slot], self.store_sem.at[slot])

    @staticmethod
    def scratch(count):
        return [pltpu.VMEM((RING, count, 3, CHUNK), jnp.bfloat16), pltpu.VMEM((GROUP, 3, INNER), jnp.float32), pltpu.SemaphoreType.DMA((RING,))]


def finish_kernel(gathered, near_0, near_1, near_2, mate, wv, mv, vv, *refs):
    outs, refs = refs[:16], refs[16:]
    packed, full, load_sem, store_sem, out_sem = refs[:5]
    units = 16 * ((TOTAL - MOVED) // GROUP)
    sources = [(ref, k, 0) for k, ref in enumerate((near_0, near_1, near_2))]
    sources += [(mate.at[k], k, 1) for k in range(3)]
    moved = MovedRing(sources, 0, (outs[0], outs[4]), refs[5:])
    rows = moved.rows

    def load(unit):
        slot = lax.rem(unit, DEPTH)
        pltpu.make_async_copy(gathered.at[unit % 16, pl.ds((unit // 16) * GROUP, GROUP)], packed.at[slot], load_sem.at[slot]).start()

    def store(unit):
        slot = lax.rem(unit, DEPTH)
        first = (unit // 16) * GROUP + MOVED
        for kind in range(1, 4):
            @pl.when((first >= STARTS[kind]) & (first < STARTS[kind] + COUNTS[kind]))
            def _(kind=kind):
                begin = (unit % 16) * (COUNTS[kind] * CHUNK) + (first - STARTS[kind]) * CHUNK
                cols = pl.ds(pl.multiple_of(begin, CHUNK), GROUP * CHUNK)
                pltpu.make_async_copy(full.at[slot], outs[4 * kind].at[:, cols], store_sem.at[slot]).start()

    def unpack(slot):
        for i in range(GROUP):
            for k in range(3):
                unpack_part(packed.at[slot, i, :, pl.ds(k * THIRD, THIRD)], full.at[slot], k * CHUNK + i * PART, rows.at[k])

    def fill(unit, _):
        load(unit)
        return 0

    lax.fori_loop(0, DEPTH, fill, 0)
    for j, src in enumerate((wv, mv, vv)):
        for kind in range(4):
            def put(i, _, kind=kind, j=j, src=src):
                cols = pl.ds(pl.multiple_of(i * CHUNK, CHUNK), CHUNK)
                pltpu.make_async_copy(src.at[STARTS[kind] + i], outs[4 * kind + 1 + j].at[:, cols], out_sem.at[j]).start()
                return 0

            lax.fori_loop(0, COUNTS[kind], put, 0)

    def step(unit, _):
        slot = lax.rem(unit, DEPTH)
        wait_for(packed.at[slot], load_sem.at[slot])

        @pl.when(unit >= DEPTH)
        def _():
            wait_for(full.at[slot], store_sem.at[slot])

        unpack(slot)
        store(unit)

        @pl.when(unit + DEPTH < units)
        def _():
            load(unit + DEPTH)

        return 0

    lax.fori_loop(0, units, step, 0)
    moved.run()

    def drain(slot, _):
        wait_for(full.at[slot], store_sem.at[slot])
        return 0

    lax.fori_loop(0, DEPTH, drain, 0)
    moved.drain()
    for j, src in enumerate((wv, mv, vv)):
        wait_for(src, out_sem.at[j])


def finish(gathered, near, mate, new_states):
    f32, bf16 = jnp.float32, jnp.bfloat16
    dma = pltpu.SemaphoreType.DMA
    any_space = pl.BlockSpec(memory_space=pl.ANY)
    shapes = []
    for count in COUNTS:
        shapes += [jax.ShapeDtypeStruct((3, 16 * count * CHUNK), bf16)] + [jax.ShapeDtypeStruct((3, count * CHUNK), f32)] * 3
    return pl.pallas_call(
        finish_kernel,
        out_shape=tuple(shapes),
        in_specs=[any_space] + [pl.BlockSpec(memory_space=pltpu.VMEM)] * 7,
        out_specs=(any_space,) * 16,
        scratch_shapes=[
            pltpu.VMEM((DEPTH, GROUP, 4, PACKED), bf16), pltpu.VMEM((DEPTH, 3, GROUP * CHUNK), bf16),
            dma((DEPTH,)), dma((DEPTH,)), dma((3,)),
        ] + MovedRing.scratch(6),
        compiler_params=pltpu.CompilerParams(vmem_limit_bytes=LAST_VMEM),
        cost_estimate=pl.CostEstimate(flops=10 ** 12, bytes_accessed=10 ** 8, transcendentals=0),
        name="finish",
    )(pltpu.with_memory_space_constraint(gathered, pltpu.HBM), *[in_vmem(x) for x in (*near, mate, *new_states)])


def far_kernel(other, *refs):
    arrays, outs, buffers = refs[:3], refs[5:7], refs[7:]
    ring = MovedRing([(ref, k, other) for k, ref in enumerate(arrays)], 1, outs, buffers)
    ring.run()
    ring.drain()


def finish_far(far, other, copies):
    any_space = pl.BlockSpec(memory_space=pl.ANY)
    return pl.pallas_call(
        functools.partial(far_kernel, other),
        out_shape=tuple(jax.ShapeDtypeStruct(x.shape, x.dtype) for x in copies),
        in_specs=[pl.BlockSpec(memory_space=pltpu.VMEM)] * 3 + [any_space] * 2,
        out_specs=(any_space,) * 2,
        scratch_shapes=MovedRing.scratch(3),
        input_output_aliases={3: 0, 4: 1},
        compiler_params=pltpu.CompilerParams(vmem_limit_bytes=FAR_VMEM),
        cost_estimate=pl.CostEstimate(flops=10 ** 11, bytes_accessed=10 ** 7, transcendentals=0),
    )(*far, *copies)


def optimizer_step(blocks):
    f32, bf16 = jnp.float32, jnp.bfloat16
    dma = pltpu.SemaphoreType.DMA
    any_space = pl.BlockSpec(memory_space=pl.ANY)
    operands = []
    for kind in KINDS:
        grad, weight, first_mom, second_mom = blocks[4 * kind:4 * kind + 4]
        operands += [grad.reshape(grad.shape[1:]), weight, first_mom, second_mom]
    part = pltpu.VMEM((4, MOVED, 4, THIRD), bf16)
    state = pltpu.VMEM((TOTAL, 3, CHUNK), f32)
    vmem_space = pl.BlockSpec(memory_space=pltpu.VMEM)
    return pl.pallas_call(
        step_kernel,
        out_shape=(pltpu.HBM((16, TOTAL - MOVED, 4, PACKED), bf16), part, part, part, pltpu.VMEM((3,) + part.shape, bf16), state, state, state),
        in_specs=[any_space] * 16,
        out_specs=(any_space,) + (vmem_space,) * 7,
        scratch_shapes=[
            pltpu.VMEM((SLOTS, 8, 3, CHUNK), bf16), pltpu.VMEM((SLOTS, 8, 3, CHUNK), bf16), pltpu.VMEM((8, 3, INNER), f32),
            pltpu.VMEM((SLOTS, 3, 4, 1, CHUNK), f32), pltpu.VMEM((SLOTS, 3, 4, 1, CHUNK), f32),
            pltpu.VMEM((SLOTS, 3, 4, 1, CHUNK), f32), pltpu.VMEM((SLOTS, 3, 2, 1, CHUNK), f32), pltpu.VMEM((SLOTS, 3, 1, 1, CHUNK), f32),
            pltpu.VMEM((TOTAL, 3, 1, CHUNK), f32),
            pltpu.VMEM((4, 6, 1, INNER), f32), pltpu.VMEM((4, 8, 128), f32), pltpu.VMEM((4, 16, 8, 128), f32), pltpu.VMEM((4, 3, 1, INNER), f32),
            pltpu.VMEM((3, 4, INNER), f32), pltpu.VMEM((TOTAL, 4, PACKED), bf16),
            dma((SLOTS,)), dma((SLOTS,)), dma((SLOTS,)),
            dma((SLOTS,)), dma((SLOTS,)), dma((SLOTS,)), dma((SLOTS,)), dma((SLOTS,)), dma((SLOTS,)),
            dma((3,)), dma((4,)), dma((4,)),
            dma, dma, dma, dma((SLOTS,)), dma((SLOTS,)), dma((SLOTS,)), dma, dma, dma, dma, dma, dma,
        ],
        compiler_params=pltpu.CompilerParams(collective_id=0, has_side_effects=True, vmem_limit_bytes=STEP_VMEM),
        name="lamb_step",
    )(*operands)


def solution(mesh):
    grad_spec = P("data", None, None)
    shard_spec = P(None, "data")
    full_spec = P(None, None)

    def device_step(*blocks):
        gathered, *near_mate = optimizer_step(blocks)
        near, mate, new_states = near_mate[:3], near_mate[3], near_mate[4:]
        far = []
        for k in range(3):
            far.append(in_vmem(lax.ppermute(near[k], "data", [(i, i ^ (2 << ORDERS[k][2])) for i in range(16)])))
        outs = list(finish(gathered, near, mate, new_states))
        far_mate = []
        for k in range(3):
            far_mate.append(in_vmem(lax.ppermute(far[k], "data", [(i, i ^ 1) for i in range(16)])))
        copies = (outs[0], outs[4])
        copies = finish_far(far, 0, copies)
        outs[0], outs[4] = finish_far(far_mate, 1, copies)
        results = [None] * 16
        for slot, kind in enumerate(KINDS):
            results[4 * kind:4 * kind + 4] = outs[4 * slot:4 * slot + 4]
        return tuple(results)

    return jax.shard_map(device_step, mesh=mesh, in_specs=(grad_spec, shard_spec, shard_spec, shard_spec) * 4, out_specs=(full_spec, shard_spec, shard_spec, shard_spec) * 4, check_vma=False)
```

```python
import functools

import jax
import jax.numpy as jnp
from jax import lax
from jax.experimental import pallas as pl
from jax.experimental.pallas import tpu as pltpu
from jax.sharding import PartitionSpec as P


STEP = 10
LEARN_RATE = 0.1
BETA_ONE = 0.9
BETA_TWO = 0.999
EPSILON = 1e-6
WEIGHT_DECAY = 0.01

MESH = pl.DeviceIdType.MESH
CHUNK = 12288
INNER = 1024
PACKED = CHUNK * 3 // 4
THIRD = PACKED // 3
PART = CHUNK // 3
SLOTS = 4
LEAD = 2
KINDS = (2, 3, 0, 1)
COUNTS = (12, 12, 9, 3)
STARTS = (0, 12, 24, 33)
TOTAL = 36
MOVED = 15
STEP_VMEM = 28 << 20
LAST_VMEM = 13 << 20
FAR_VMEM = 6 << 20
PACK_AT = 17
GROUP = 3
DEPTH = 12
RING = 4
ORDERS = ((0, 1, 2), (1, 2, 0), (2, 0, 1))


def kind_of(chunk):
    return sum(jnp.where(chunk >= start, 1, 0) for start in STARTS[1:])


def step_kernel(*refs):
    states, refs = refs[:16], refs[16:]
    (gathered, near_0, near_1, near_2, mate, wv, mv, vv,
     own, peer, pair, send1, keep, recv1, recv2, recv3, uv, acc, part, parts, ratio, quad, packed,
     own_sem, peer_send, peer_recv, s1, r1, s2, r2, s3, r3, state_sem, part_send, part_recv,
     a1s, a2s, a3s, a1r, a2r, a3r, self_sem, mate_send, mate_recv, a2n, near_send, near_recv) = refs
    near = (near_0, near_1, near_2)
    me = lax.axis_index("data")
    core = me % 2
    bits = ((me // 2) % 2, (me // 4) % 2, (me // 8) % 2)
    partner = me + 1 - 2 * core
    neighbour = tuple(me + (2 << d) * (1 - 2 * bits[d]) for d in range(3))

    def owner(rel, parity):
        index = parity
        for d in range(3):
            index = index + (2 << d) * (1 - bits[d] if (rel >> d) & 1 else bits[d])
        return index

    def remote(src, dst, ssem, rsem, device):
        return pltpu.make_async_remote_copy(src_ref=src, dst_ref=dst, send_sem=ssem, recv_sem=rsem,
                                            device_id=(device,), device_id_type=MESH)

    def wait_for(ref, sem):
        pltpu.make_async_copy(ref, ref, sem).wait()

    def slot_of(chunk):
        return lax.rem(chunk, SLOTS)

    def for_kind(chunk, body):
        for kind in range(4):
            @pl.when((chunk >= STARTS[kind]) & (chunk < STARTS[kind] + COUNTS[kind]))
            def _(kind=kind):
                body(kind, chunk - STARTS[kind])

    def load_own(chunk):
        def body(kind, local):
            width = COUNTS[kind] * CHUNK
            slot = slot_of(chunk)
            for i in range(3):
                for rel in range(8):
                    cols = pl.ds(pl.multiple_of(owner(rel, core) * width + local * CHUNK + i * PART, 128), PART)
                    pltpu.make_async_copy(states[4 * kind].at[:, cols], own.at[slot, rel, :, pl.ds(i * PART, PART)], own_sem.at[slot, i]).start()

        for_kind(chunk, body)

    def give_peer(chunk):
        def body(kind, local):
            width = COUNTS[kind] * CHUNK
            slot = slot_of(chunk)
            for i in range(3):
                for rel in range(8):
                    cols = pl.ds(pl.multiple_of(owner(rel, 1 - core) * width + local * CHUNK + i * PART, 128), PART)
                    remote(states[4 * kind].at[:, cols], peer.at[slot, rel, :, pl.ds(i * PART, PART)], peer_send.at[slot], peer_recv.at[slot, i], partner).start()

        for_kind(chunk, body)

    def pair_stage(chunk):
        slot = slot_of(chunk)

        @pl.when(chunk >= SLOTS)
        def _():
            wait_for(send1.at[slot], s1.at[slot])
            wait_for(recv2.at[slot], s2.at[slot])
            wait_for(recv3.at[slot], s3.at[slot])

        def one_part(n, _):
            cols = pl.ds(pl.multiple_of(n * PART, PART), PART)
            wait_for(own.at[slot, :, :, cols], own_sem.at[slot, n])
            wait_for(peer.at[slot, :, :, cols], peer_recv.at[slot, n])
            for rel in range(8):
                def inner(i, _, rel=rel):
                    cols = pl.ds(pl.multiple_of(n * PART + i * INNER, INNER), INNER)
                    pair[rel] = own[slot, rel, :, cols].astype(jnp.float32) + peer[slot, rel, :, cols].astype(jnp.float32)
                    for row in range(3):
                        a, b, c = ((rel >> d) & 1 for d in ORDERS[row])
                        dst = send1 if a else keep
                        dst[slot, row, 2 * b + c, :, cols] = pair[rel, row:row + 1, :]
                    return 0

                lax.fori_loop(0, PART // INNER, inner, 0)
            for row in range(3):
                remote(send1.at[slot, row, :, :, cols], recv1.at[slot, row, :, :, cols], s1.at[slot], r1.at[slot], neighbour[ORDERS[row][0]]).start()
            return 0

        lax.fori_loop(0, 3, one_part, 0)

    def prefetch(chunk):
        @pl.when(chunk >= SLOTS)
        def _():
            wait_for(peer.at[slot_of(chunk)], peer_send.at[slot_of(chunk)])

        load_own(chunk)
        give_peer(chunk)

    def add_stage(slot, recv, rsem, count):
        wait_for(recv.at[slot], rsem.at[slot])

        def inner(i, _):
            cols = pl.ds(pl.multiple_of(i * INNER, INNER), INNER)
            for row in range(3):
                for k in range(count):
                    keep[slot, row, k, :, cols] = keep[slot, row, k, :, cols] + recv[slot, row, k, :, cols]
            return 0

        lax.fori_loop(0, CHUNK // INNER, inner, 0)

    def second_stage(chunk):
        slot = slot_of(chunk)
        add_stage(slot, recv1, r1, 4)
        for row in range(3):
            remote(keep.at[slot, row, pl.ds(2, 2)], recv2.at[slot, row], s2.at[slot], r2.at[slot], neighbour[ORDERS[row][1]]).start()

    def third_stage(chunk):
        slot = slot_of(chunk)
        add_stage(slot, recv2, r2, 2)
        for row in range(3):
            remote(keep.at[slot, row, pl.ds(1, 1)], recv3.at[slot, row], s3.at[slot], r3.at[slot], neighbour[ORDERS[row][2]]).start()

    def last_stage(chunk):
        slot = slot_of(chunk)
        kind = kind_of(chunk)
        wait_for(recv3.at[slot], r3.at[slot])

        def inner(i, _):
            cols = pl.ds(pl.multiple_of(i * INNER, INNER), INNER)
            for row in range(3):
                line = slice(row, row + 1)
                mean = (keep[slot, row, 0, :, cols] + recv3[slot, row, 0, :, cols]) / 16
                weight = wv[chunk, line, cols]
                new_first = BETA_ONE * mv[chunk, line, cols] + (1.0 - BETA_ONE) * mean
                new_second = BETA_TWO * vv[chunk, line, cols] + (1.0 - BETA_TWO) * mean * mean
                direction = (new_first / (1.0 - BETA_ONE ** STEP)) / (jnp.sqrt(new_second / (1.0 - BETA_TWO ** STEP)) + EPSILON) + WEIGHT_DECAY * weight
                mv[chunk, line, cols] = new_first
                vv[chunk, line, cols] = new_second
                uv[chunk, row, :, cols] = direction
                acc[kind, row] += weight * weight
                acc[kind, 3 + row] += direction * direction
            return 0

        lax.fori_loop(0, CHUNK // INNER, inner, 0)

    def send_norms(kind):
        for j in range(6):
            part[kind, j:j + 1, :] = jnp.broadcast_to(jnp.sum(acc[kind, j], axis=1, keepdims=True), (1, 128))
        for j in range(6, 8):
            part[kind, j:j + 1, :] = jnp.zeros((1, 128), jnp.float32)
        parts[kind, me] = part[kind]
        for k in range(1, 16):
            remote(part.at[kind], parts.at[kind, me], part_send.at[kind], part_recv.at[kind], (me + k) % 16).start()

    def take_norms(kind):
        wait_for(parts.at[kind, pl.ds(0, 15)], part_recv.at[kind])
        total = parts[kind, 0]
        for i in range(1, 16):
            total = total + parts[kind, i]
        norms = jnp.sqrt(total)
        trust = norms[0:3, :] / norms[3:6, :]
        for row in range(3):
            for i in range(INNER // 128):
                ratio[kind, row, :, i * 128:(i + 1) * 128] = trust[row:row + 1, :]

    def update(chunk):
        kind = kind_of(chunk)

        def inner(i, _):
            cols = pl.ds(pl.multiple_of(i * INNER, INNER), INNER)
            for row in range(3):
                line = slice(row, row + 1)
                wv[chunk, line, cols] = wv[chunk, line, cols] - LEARN_RATE * ratio[kind, row] * uv[chunk, row, :, cols]
            return 0

        lax.fori_loop(0, CHUNK // INNER, inner, 0)

    def pack(unit):
        begin = lax.rem(unit, GROUP) * PART
        for k in range(3):
            chunk = unit - lax.rem(unit, GROUP) + k
            for row in range(3):
                head = pl.ds(pl.multiple_of(begin + row * INNER, INNER), INNER)
                tail = pl.ds(pl.multiple_of(begin + THIRD, INNER), INNER)
                quad[row, 0:3, :] = wv[chunk, :, head]
                quad[row, 3:4, :] = wv[chunk, row:row + 1, tail]
                packed[unit, :, k * THIRD + row * INNER:k * THIRD + (row + 1) * INNER] = quad[row].astype(jnp.bfloat16)

    def thirds(k):
        return pl.ds(k * THIRD, THIRD)

    def offset(*dims):
        return sum(1 << d for d in dims)

    def piece(rel, chunk, k):
        return gathered.at[owner(rel, core), chunk - MOVED, :, thirds(k)]

    def to_partner(rel, chunk, k):
        remote(piece(rel, chunk, k), piece(rel, chunk, k), mate_send, mate_recv, partner).start()

    def near_to_partner(k, j, chunk):
        remote(near[k].at[j, chunk], mate.at[k, j, chunk], near_send, near_recv, partner).start()

    def gather_one(chunk):
        slot = slot_of(chunk)

        @pl.when(chunk < MOVED)
        def _():
            for k in range(3):
                mine = packed.at[chunk, :, thirds(k)]
                remote(mine, near[k].at[1, chunk], a1s, a1r.at[slot], neighbour[ORDERS[k][0]]).start()
                remote(mine, mate.at[k, 0, chunk], near_send, near_recv, partner).start()
                pltpu.make_async_copy(mine, near[k].at[0, chunk], self_sem).start()

        @pl.when(chunk >= MOVED)
        def _():
            for k in range(3):
                remote(packed.at[chunk, :, thirds(k)], piece(0, chunk, k), a1s, a1r.at[slot], neighbour[ORDERS[k][0]]).start()
            mine = gathered.at[me, chunk - MOVED]
            remote(packed.at[chunk], mine, mate_send, mate_recv, partner).start()
            pltpu.make_async_copy(packed.at[chunk], mine, self_sem).start()

    def gather_two(chunk):
        slot = slot_of(chunk)
        wait_for(packed.at[0], a1r.at[slot])

        @pl.when(chunk < MOVED)
        def _():
            for k in range(3):
                device = neighbour[ORDERS[k][1]]
                remote(packed.at[chunk, :, thirds(k)], near[k].at[2, chunk], a2n, a2r.at[slot], device).start()
                remote(near[k].at[1, chunk], near[k].at[3, chunk], a2n, a2r.at[slot], device).start()
            for k in range(3):
                near_to_partner(k, 1, chunk)

        @pl.when(chunk >= MOVED)
        def _():
            for k in range(3):
                a, b, _ = ORDERS[k]
                remote(packed.at[chunk, :, thirds(k)], piece(0, chunk, k), a2s, a2r.at[slot], neighbour[b]).start()
                remote(piece(offset(a), chunk, k), piece(offset(a), chunk, k), a2s, a2r.at[slot], neighbour[b]).start()
            for k in range(3):
                to_partner(offset(ORDERS[k][0]), chunk, k)

    def gather_three(chunk):
        slot = slot_of(chunk)
        wait_for(packed.at[pl.ds(0, 2)], a2r.at[slot])

        @pl.when(chunk < MOVED)
        def _():
            for k in range(3):
                near_to_partner(k, 2, chunk)
                near_to_partner(k, 3, chunk)

        @pl.when(chunk >= MOVED)
        def _():
            for k in range(3):
                a, b, c = ORDERS[k]
                remote(packed.at[chunk, :, thirds(k)], piece(0, chunk, k), a3s, a3r.at[slot], neighbour[c]).start()
                for rel in (offset(a), offset(b), offset(a, b)):
                    remote(piece(rel, chunk, k), piece(rel, chunk, k), a3s, a3r.at[slot], neighbour[c]).start()
            for k in range(3):
                a, b, c = ORDERS[k]
                to_partner(offset(b), chunk, k)
                to_partner(offset(a, b), chunk, k)

    def gather_four(chunk):
        @pl.when(chunk >= MOVED)
        def _():
            wait_for(packed.at[pl.ds(0, 4)], a3r.at[slot_of(chunk)])
            for k in range(3):
                a, b, c = ORDERS[k]
                for rel in (offset(c), offset(a, c), offset(b, c), offset(a, b, c)):
                    to_partner(rel, chunk, k)

    def at_chunk(chunk, body):
        @pl.when((chunk >= 0) & (chunk < TOTAL))
        def _():
            body(chunk)

    load_own(jnp.int32(0))
    load_own(jnp.int32(1))
    barrier = pltpu.get_barrier_semaphore()
    for k in range(1, 16):
        pl.semaphore_signal(barrier, inc=1, device_id=((me + k) % 16,), device_id_type=MESH)
    pl.semaphore_wait(barrier, 15)
    give_peer(jnp.int32(0))
    give_peer(jnp.int32(1))
    acc[...] = jnp.zeros_like(acc)

    def step(s, _):
        at_chunk(s, pair_stage)

        @pl.when(s + LEAD < TOTAL)
        def _():
            prefetch(s + LEAD)

        @pl.when(s == 0)
        def _():
            for kind in range(4):
                def load_states(i, _, kind=kind):
                    cols = pl.ds(pl.multiple_of(i * CHUNK, CHUNK), CHUNK)
                    for j, dst in enumerate((wv, mv, vv)):
                        pltpu.make_async_copy(states[4 * kind + 1 + j].at[:, cols], dst.at[STARTS[kind] + i], state_sem.at[j]).start()
                    return 0

                lax.fori_loop(0, COUNTS[kind], load_states, 0)

        at_chunk(s - 1, second_stage)
        at_chunk(s - 2, third_stage)

        @pl.when(s == 3)
        def _():
            for j, dst in enumerate((wv, mv, vv)):
                wait_for(dst, state_sem.at[j])

        at_chunk(s - 3, last_stage)
        for kind in range(4):
            @pl.when(s == STARTS[kind] + COUNTS[kind] + 2)
            def _(kind=kind):
                send_norms(kind)

            @pl.when(s == PACK_AT - 2 + STARTS[kind])
            def _(kind=kind):
                take_norms(kind)
        at_chunk(s - PACK_AT - 1, gather_one)
        at_chunk(s - PACK_AT - 2, gather_two)
        at_chunk(s - PACK_AT - 3, gather_three)
        at_chunk(s - PACK_AT - 4, gather_four)
        at_chunk(s - PACK_AT + 2, update)
        at_chunk(s - PACK_AT, pack)
        return 0

    lax.fori_loop(0, TOTAL + PACK_AT + 5, step, 0)

    def drain(chunk, _):
        slot = slot_of(chunk)
        wait_for(peer.at[slot], peer_send.at[slot])
        wait_for(send1.at[slot], s1.at[slot])
        wait_for(recv2.at[slot], s2.at[slot])
        wait_for(recv3.at[slot], s3.at[slot])
        return 0

    lax.fori_loop(TOTAL - SLOTS, TOTAL, drain, 0)
    for kind in range(4):
        wait_for(parts.at[kind, pl.ds(0, 15)], part_send.at[kind])
    wait_for(packed, a1s)
    wait_for(packed, self_sem)
    wait_for(gathered.at[pl.ds(0, 2)], a2s)
    wait_for(mate.at[:, pl.ds(0, 2)], a2n)
    wait_for(gathered.at[pl.ds(0, 4)], a3s)
    for sem in (mate_send, mate_recv):
        wait_for(gathered.at[pl.ds(0, 8)], sem)
    for sem in (near_send, near_recv):
        wait_for(mate, sem)


def wait_for(ref, sem):
    pltpu.make_async_copy(ref, ref, sem).wait()


def in_vmem(x):
    return pltpu.with_memory_space_constraint(x, pltpu.VMEM)


def unpack_part(src, dst, col, rows):
    dst[:, pl.ds(col, THIRD)] = src[0:3, :]
    for row in range(3):
        rows[row:row + 1, :] = src[3:4, row * INNER:(row + 1) * INNER].astype(jnp.float32)
    dst[:, pl.ds(col + THIRD, INNER)] = rows[...].astype(jnp.bfloat16)


class MovedRing:
    def __init__(self, sources, far, outs, buffers):
        self.sources, self.far, self.outs = sources, far, outs
        self.full, self.rows, self.store_sem = buffers
        self.groups = MOVED // GROUP
        self.steps = 4 * self.groups
        me = lax.axis_index("data")
        self.core = me % 2
        self.bits = ((me // 2) % 2, (me // 4) % 2, (me // 8) % 2)

    def store(self, step):
        slot = lax.rem(step, RING)
        j, group = step // self.groups, lax.rem(step, self.groups)
        for i, (_, k, other) in enumerate(self.sources):
            rel = [0, 0, 0]
            for d, bit in zip(ORDERS[k], (j % 2, j // 2, self.far)):
                rel[d] = bit
            shard = self.core + other - 2 * other * self.core
            for d in range(3):
                shard = shard + (2 << d) * (self.bits[d] + rel[d] - 2 * self.bits[d] * rel[d])
            for kind in range(2):
                @pl.when((group >= COUNTS[0] // GROUP) if kind else (group < COUNTS[0] // GROUP))
                def _(kind=kind, i=i, k=k, shard=shard):
                    begin = (shard * COUNTS[kind] + group * GROUP + k - STARTS[kind]) * CHUNK
                    pltpu.make_async_copy(self.full.at[slot, i], self.outs[kind].at[:, pl.ds(pl.multiple_of(begin, CHUNK), CHUNK)],
                                          self.store_sem.at[slot]).start()

    def run(self):
        def body(step, _):
            slot = lax.rem(step, RING)

            @pl.when(step >= RING)
            def _():
                wait_for(self.full.at[slot], self.store_sem.at[slot])

            j, first = step // self.groups, lax.rem(step, self.groups) * GROUP
            for i, (source, _, _) in enumerate(self.sources):
                for c in range(GROUP):
                    unpack_part(source.at[j, first + c], self.full.at[slot, i], c * PART, self.rows.at[c])
            self.store(step)
            return 0

        lax.fori_loop(0, self.steps, body, 0)

    def drain(self):
        for slot in range(RING):
            wait_for(self.full.at[slot], self.store_sem.at[slot])

    @staticmethod
    def scratch(count):
        return [pltpu.VMEM((RING, count, 3, CHUNK), jnp.bfloat16), pltpu.VMEM((GROUP, 3, INNER), jnp.float32), pltpu.SemaphoreType.DMA((RING,))]


def finish_kernel(gathered, near_0, near_1, near_2, mate, wv, mv, vv, *refs):
    outs, refs = refs[:16], refs[16:]
    packed, full, load_sem, store_sem, out_sem = refs[:5]
    units = 16 * ((TOTAL - MOVED) // GROUP)
    sources = [(ref, k, 0) for k, ref in enumerate((near_0, near_1, near_2))]
    sources += [(mate.at[k], k, 1) for k in range(3)]
    moved = MovedRing(sources, 0, (outs[0], outs[4]), refs[5:])
    rows = moved.rows

    def load(unit):
        slot = lax.rem(unit, DEPTH)
        pltpu.make_async_copy(gathered.at[unit % 16, pl.ds((unit // 16) * GROUP, GROUP)], packed.at[slot], load_sem.at[slot]).start()

    def store(unit):
        slot = lax.rem(unit, DEPTH)
        first = (unit // 16) * GROUP + MOVED
        for kind in range(1, 4):
            @pl.when((first >= STARTS[kind]) & (first < STARTS[kind] + COUNTS[kind]))
            def _(kind=kind):
                begin = (unit % 16) * (COUNTS[kind] * CHUNK) + (first - STARTS[kind]) * CHUNK
                cols = pl.ds(pl.multiple_of(begin, CHUNK), GROUP * CHUNK)
                pltpu.make_async_copy(full.at[slot], outs[4 * kind].at[:, cols], store_sem.at[slot]).start()

    def unpack(slot):
        for i in range(GROUP):
            for k in range(3):
                unpack_part(packed.at[slot, i, :, pl.ds(k * THIRD, THIRD)], full.at[slot], k * CHUNK + i * PART, rows.at[k])

    def fill(unit, _):
        load(unit)
        return 0

    lax.fori_loop(0, DEPTH, fill, 0)
    for j, src in enumerate((wv, mv, vv)):
        for kind in range(4):
            def put(i, _, kind=kind, j=j, src=src):
                cols = pl.ds(pl.multiple_of(i * CHUNK, CHUNK), CHUNK)
                pltpu.make_async_copy(src.at[STARTS[kind] + i], outs[4 * kind + 1 + j].at[:, cols], out_sem.at[j]).start()
                return 0

            lax.fori_loop(0, COUNTS[kind], put, 0)

    def step(unit, _):
        slot = lax.rem(unit, DEPTH)
        wait_for(packed.at[slot], load_sem.at[slot])

        @pl.when(unit >= DEPTH)
        def _():
            wait_for(full.at[slot], store_sem.at[slot])

        unpack(slot)
        store(unit)

        @pl.when(unit + DEPTH < units)
        def _():
            load(unit + DEPTH)

        return 0

    lax.fori_loop(0, units, step, 0)
    moved.run()

    def drain(slot, _):
        wait_for(full.at[slot], store_sem.at[slot])
        return 0

    lax.fori_loop(0, DEPTH, drain, 0)
    moved.drain()
    for j, src in enumerate((wv, mv, vv)):
        wait_for(src, out_sem.at[j])


def finish(gathered, near, mate, new_states):
    f32, bf16 = jnp.float32, jnp.bfloat16
    dma = pltpu.SemaphoreType.DMA
    any_space = pl.BlockSpec(memory_space=pl.ANY)
    shapes = []
    for count in COUNTS:
        shapes += [jax.ShapeDtypeStruct((3, 16 * count * CHUNK), bf16)] + [jax.ShapeDtypeStruct((3, count * CHUNK), f32)] * 3
    return pl.pallas_call(
        finish_kernel,
        out_shape=tuple(shapes),
        in_specs=[any_space] + [pl.BlockSpec(memory_space=pltpu.VMEM)] * 7,
        out_specs=(any_space,) * 16,
        scratch_shapes=[
            pltpu.VMEM((DEPTH, GROUP, 4, PACKED), bf16), pltpu.VMEM((DEPTH, 3, GROUP * CHUNK), bf16),
            dma((DEPTH,)), dma((DEPTH,)), dma((3,)),
        ] + MovedRing.scratch(6),
        compiler_params=pltpu.CompilerParams(vmem_limit_bytes=LAST_VMEM),
        cost_estimate=pl.CostEstimate(flops=10 ** 12, bytes_accessed=10 ** 8, transcendentals=0),
        name="finish",
    )(pltpu.with_memory_space_constraint(gathered, pltpu.HBM), *[in_vmem(x) for x in (*near, mate, *new_states)])


def far_kernel(other, *refs):
    arrays, outs, buffers = refs[:3], refs[5:7], refs[7:]
    ring = MovedRing([(ref, k, other) for k, ref in enumerate(arrays)], 1, outs, buffers)
    ring.run()
    ring.drain()


def finish_far(far, other, copies):
    any_space = pl.BlockSpec(memory_space=pl.ANY)
    return pl.pallas_call(
        functools.partial(far_kernel, other),
        out_shape=tuple(jax.ShapeDtypeStruct(x.shape, x.dtype) for x in copies),
        in_specs=[pl.BlockSpec(memory_space=pltpu.VMEM)] * 3 + [any_space] * 2,
        out_specs=(any_space,) * 2,
        scratch_shapes=MovedRing.scratch(3),
        input_output_aliases={3: 0, 4: 1},
        compiler_params=pltpu.CompilerParams(vmem_limit_bytes=FAR_VMEM),
        cost_estimate=pl.CostEstimate(flops=10 ** 11, bytes_accessed=10 ** 7, transcendentals=0),
    )(*far, *copies)


def optimizer_step(blocks):
    f32, bf16 = jnp.float32, jnp.bfloat16
    dma = pltpu.SemaphoreType.DMA
    any_space = pl.BlockSpec(memory_space=pl.ANY)
    operands = []
    for kind in KINDS:
        grad, weight, first_mom, second_mom = blocks[4 * kind:4 * kind + 4]
        operands += [grad.reshape(grad.shape[1:]), weight, first_mom, second_mom]
    part = pltpu.VMEM((4, MOVED, 4, THIRD), bf16)
    state = pltpu.VMEM((TOTAL, 3, CHUNK), f32)
    vmem_space = pl.BlockSpec(memory_space=pltpu.VMEM)
    return pl.pallas_call(
        step_kernel,
        out_shape=(pltpu.HBM((16, TOTAL - MOVED, 4, PACKED), bf16), part, part, part, pltpu.VMEM((3,) + part.shape, bf16), state, state, state),
        in_specs=[any_space] * 16,
        out_specs=(any_space,) + (vmem_space,) * 7,
        scratch_shapes=[
            pltpu.VMEM((SLOTS, 8, 3, CHUNK), bf16), pltpu.VMEM((SLOTS, 8, 3, CHUNK), bf16), pltpu.VMEM((8, 3, INNER), f32),
            pltpu.VMEM((SLOTS, 3, 4, 1, CHUNK), f32), pltpu.VMEM((SLOTS, 3, 4, 1, CHUNK), f32),
            pltpu.VMEM((SLOTS, 3, 4, 1, CHUNK), f32), pltpu.VMEM((SLOTS, 3, 2, 1, CHUNK), f32), pltpu.VMEM((SLOTS, 3, 1, 1, CHUNK), f32),
            pltpu.VMEM((TOTAL, 3, 1, CHUNK), f32),
            pltpu.VMEM((4, 6, 1, INNER), f32), pltpu.VMEM((4, 8, 128), f32), pltpu.VMEM((4, 16, 8, 128), f32), pltpu.VMEM((4, 3, 1, INNER), f32),
            pltpu.VMEM((3, 4, INNER), f32), pltpu.VMEM((TOTAL, 4, PACKED), bf16),
            dma((SLOTS, 3)), dma((SLOTS,)), dma((SLOTS, 3)),
            dma((SLOTS,)), dma((SLOTS,)), dma((SLOTS,)), dma((SLOTS,)), dma((SLOTS,)), dma((SLOTS,)),
            dma((3,)), dma((4,)), dma((4,)),
            dma, dma, dma, dma((SLOTS,)), dma((SLOTS,)), dma((SLOTS,)), dma, dma, dma, dma, dma, dma,
        ],
        compiler_params=pltpu.CompilerParams(collective_id=0, has_side_effects=True, vmem_limit_bytes=STEP_VMEM),
        name="lamb_step",
    )(*operands)


def solution(mesh):
    grad_spec = P("data", None, None)
    shard_spec = P(None, "data")
    full_spec = P(None, None)

    def device_step(*blocks):
        gathered, *near_mate = optimizer_step(blocks)
        near, mate, new_states = near_mate[:3], near_mate[3], near_mate[4:]
        far = []
        for k in range(3):
            far.append(in_vmem(lax.ppermute(near[k], "data", [(i, i ^ (2 << ORDERS[k][2])) for i in range(16)])))
        outs = list(finish(gathered, near, mate, new_states))
        far_mate = []
        for k in range(3):
            far_mate.append(in_vmem(lax.ppermute(far[k], "data", [(i, i ^ 1) for i in range(16)])))
        copies = (outs[0], outs[4])
        copies = finish_far(far, 0, copies)
        outs[0], outs[4] = finish_far(far_mate, 1, copies)
        results = [None] * 16
        for slot, kind in enumerate(KINDS):
            results[4 * kind:4 * kind + 4] = outs[4 * slot:4 * slot + 4]
        return tuple(results)

    return jax.shard_map(device_step, mesh=mesh, in_specs=(grad_spec, shard_spec, shard_spec, shard_spec) * 4, out_specs=(full_spec, shard_spec, shard_spec, shard_spec) * 4, check_vma=False)
```

```python
import functools

import jax
import jax.numpy as jnp
from jax import lax
from jax.experimental import pallas as pl
from jax.experimental.pallas import tpu as pltpu
from jax.sharding import PartitionSpec as P


STEP = 10
LEARN_RATE = 0.1
BETA_ONE = 0.9
BETA_TWO = 0.999
EPSILON = 1e-6
WEIGHT_DECAY = 0.01

MESH = pl.DeviceIdType.MESH
CHUNK = 12288
INNER = 1024
PACKED = CHUNK * 3 // 4
THIRD = PACKED // 3
PART = CHUNK // 3
SLOTS = 4
LEAD = 2
KINDS = (2, 3, 0, 1)
COUNTS = (12, 12, 9, 3)
STARTS = (0, 12, 24, 33)
TOTAL = 36
MOVED = 15
STEP_VMEM = 28 << 20
LAST_VMEM = 13 << 20
FAR_VMEM = 9 << 20
PACK_AT = 17
GROUP = 3
DEPTH = 9
RING = 6
FAR_RING = 9
ORDERS = ((0, 1, 2), (1, 2, 0), (2, 0, 1))


def kind_of(chunk):
    return sum(jnp.where(chunk >= start, 1, 0) for start in STARTS[1:])


def step_kernel(*refs):
    states, refs = refs[:16], refs[16:]
    (gathered, near_0, near_1, near_2, mate, wv, mv, vv,
     own, peer, pair, send1, keep, recv1, recv2, recv3, uv, acc, part, parts, ratio, quad, packed,
     own_sem, peer_send, peer_recv, s1, r1, s2, r2, s3, r3, state_sem, part_send, part_recv,
     a1s, a2s, a3s, a1r, a2r, a3r, self_sem, mate_send, mate_recv, a2n, near_send, near_recv) = refs
    near = (near_0, near_1, near_2)
    me = lax.axis_index("data")
    core = me % 2
    bits = ((me // 2) % 2, (me // 4) % 2, (me // 8) % 2)
    partner = me + 1 - 2 * core
    neighbour = tuple(me + (2 << d) * (1 - 2 * bits[d]) for d in range(3))

    def owner(rel, parity):
        index = parity
        for d in range(3):
            index = index + (2 << d) * (1 - bits[d] if (rel >> d) & 1 else bits[d])
        return index

    def remote(src, dst, ssem, rsem, device):
        return pltpu.make_async_remote_copy(src_ref=src, dst_ref=dst, send_sem=ssem, recv_sem=rsem,
                                            device_id=(device,), device_id_type=MESH)

    def wait_for(ref, sem):
        pltpu.make_async_copy(ref, ref, sem).wait()

    def slot_of(chunk):
        return lax.rem(chunk, SLOTS)

    def for_kind(chunk, body):
        for kind in range(4):
            @pl.when((chunk >= STARTS[kind]) & (chunk < STARTS[kind] + COUNTS[kind]))
            def _(kind=kind):
                body(kind, chunk - STARTS[kind])

    def load_own(chunk):
        def body(kind, local):
            width = COUNTS[kind] * CHUNK
            slot = slot_of(chunk)
            for i in range(3):
                for rel in range(8):
                    cols = pl.ds(pl.multiple_of(owner(rel, core) * width + local * CHUNK + i * PART, 128), PART)
                    pltpu.make_async_copy(states[4 * kind].at[:, cols], own.at[slot, rel, :, pl.ds(i * PART, PART)], own_sem.at[slot, i]).start()

        for_kind(chunk, body)

    def give_peer(chunk):
        def body(kind, local):
            width = COUNTS[kind] * CHUNK
            slot = slot_of(chunk)
            for i in range(3):
                for rel in range(8):
                    cols = pl.ds(pl.multiple_of(owner(rel, 1 - core) * width + local * CHUNK + i * PART, 128), PART)
                    remote(states[4 * kind].at[:, cols], peer.at[slot, rel, :, pl.ds(i * PART, PART)], peer_send.at[slot], peer_recv.at[slot, i], partner).start()

        for_kind(chunk, body)

    def pair_stage(chunk):
        slot = slot_of(chunk)

        @pl.when(chunk >= SLOTS)
        def _():
            wait_for(send1.at[slot], s1.at[slot])
            wait_for(recv2.at[slot], s2.at[slot])
            wait_for(recv3.at[slot], s3.at[slot])

        def one_part(n, _):
            cols = pl.ds(pl.multiple_of(n * PART, PART), PART)
            wait_for(own.at[slot, :, :, cols], own_sem.at[slot, n])
            wait_for(peer.at[slot, :, :, cols], peer_recv.at[slot, n])
            for rel in range(8):
                def inner(i, _, rel=rel):
                    cols = pl.ds(pl.multiple_of(n * PART + i * INNER, INNER), INNER)
                    pair[rel] = own[slot, rel, :, cols].astype(jnp.float32) + peer[slot, rel, :, cols].astype(jnp.float32)
                    for row in range(3):
                        a, b, c = ((rel >> d) & 1 for d in ORDERS[row])
                        dst = send1 if a else keep
                        dst[slot, row, 2 * b + c, :, cols] = pair[rel, row:row + 1, :]
                    return 0

                lax.fori_loop(0, PART // INNER, inner, 0)
            for row in range(3):
                remote(send1.at[slot, row, :, :, cols], recv1.at[slot, row, :, :, cols], s1.at[slot], r1.at[slot], neighbour[ORDERS[row][0]]).start()
            return 0

        lax.fori_loop(0, 3, one_part, 0)

    def prefetch(chunk):
        @pl.when(chunk >= SLOTS)
        def _():
            wait_for(peer.at[slot_of(chunk)], peer_send.at[slot_of(chunk)])

        load_own(chunk)
        give_peer(chunk)

    def add_stage(slot, recv, rsem, count):
        wait_for(recv.at[slot], rsem.at[slot])

        def inner(i, _):
            cols = pl.ds(pl.multiple_of(i * INNER, INNER), INNER)
            for row in range(3):
                for k in range(count):
                    keep[slot, row, k, :, cols] = keep[slot, row, k, :, cols] + recv[slot, row, k, :, cols]
            return 0

        lax.fori_loop(0, CHUNK // INNER, inner, 0)

    def second_stage(chunk):
        slot = slot_of(chunk)
        add_stage(slot, recv1, r1, 4)
        for row in range(3):
            remote(keep.at[slot, row, pl.ds(2, 2)], recv2.at[slot, row], s2.at[slot], r2.at[slot], neighbour[ORDERS[row][1]]).start()

    def third_stage(chunk):
        slot = slot_of(chunk)
        add_stage(slot, recv2, r2, 2)
        for row in range(3):
            remote(keep.at[slot, row, pl.ds(1, 1)], recv3.at[slot, row], s3.at[slot], r3.at[slot], neighbour[ORDERS[row][2]]).start()

    def last_stage(chunk):
        slot = slot_of(chunk)
        kind = kind_of(chunk)
        wait_for(recv3.at[slot], r3.at[slot])

        def inner(i, _):
            cols = pl.ds(pl.multiple_of(i * INNER, INNER), INNER)
            for row in range(3):
                line = slice(row, row + 1)
                mean = (keep[slot, row, 0, :, cols] + recv3[slot, row, 0, :, cols]) / 16
                weight = wv[chunk, line, cols]
                new_first = BETA_ONE * mv[chunk, line, cols] + (1.0 - BETA_ONE) * mean
                new_second = BETA_TWO * vv[chunk, line, cols] + (1.0 - BETA_TWO) * mean * mean
                direction = (new_first / (1.0 - BETA_ONE ** STEP)) / (jnp.sqrt(new_second / (1.0 - BETA_TWO ** STEP)) + EPSILON) + WEIGHT_DECAY * weight
                mv[chunk, line, cols] = new_first
                vv[chunk, line, cols] = new_second
                uv[chunk, row, :, cols] = direction
                acc[kind, row] += weight * weight
                acc[kind, 3 + row] += direction * direction
            return 0

        lax.fori_loop(0, CHUNK // INNER, inner, 0)

    def send_norms(kind):
        for j in range(6):
            part[kind, j:j + 1, :] = jnp.broadcast_to(jnp.sum(acc[kind, j], axis=1, keepdims=True), (1, 128))
        for j in range(6, 8):
            part[kind, j:j + 1, :] = jnp.zeros((1, 128), jnp.float32)
        parts[kind, me] = part[kind]
        for k in range(1, 16):
            remote(part.at[kind], parts.at[kind, me], part_send.at[kind], part_recv.at[kind], (me + k) % 16).start()

    def take_norms(kind):
        wait_for(parts.at[kind, pl.ds(0, 15)], part_recv.at[kind])
        total = parts[kind, 0]
        for i in range(1, 16):
            total = total + parts[kind, i]
        norms = jnp.sqrt(total)
        trust = norms[0:3, :] / norms[3:6, :]
        for row in range(3):
            for i in range(INNER // 128):
                ratio[kind, row, :, i * 128:(i + 1) * 128] = trust[row:row + 1, :]

    def update(chunk):
        kind = kind_of(chunk)

        def inner(i, _):
            cols = pl.ds(pl.multiple_of(i * INNER, INNER), INNER)
            for row in range(3):
                line = slice(row, row + 1)
                wv[chunk, line, cols] = wv[chunk, line, cols] - LEARN_RATE * ratio[kind, row] * uv[chunk, row, :, cols]
            return 0

        lax.fori_loop(0, CHUNK // INNER, inner, 0)

    def pack(unit):
        begin = lax.rem(unit, GROUP) * PART
        for k in range(3):
            chunk = unit - lax.rem(unit, GROUP) + k
            for row in range(3):
                head = pl.ds(pl.multiple_of(begin + row * INNER, INNER), INNER)
                tail = pl.ds(pl.multiple_of(begin + THIRD, INNER), INNER)
                quad[row, 0:3, :] = wv[chunk, :, head]
                quad[row, 3:4, :] = wv[chunk, row:row + 1, tail]
                packed[unit, :, k * THIRD + row * INNER:k * THIRD + (row + 1) * INNER] = quad[row].astype(jnp.bfloat16)

    def thirds(k):
        return pl.ds(k * THIRD, THIRD)

    def offset(*dims):
        return sum(1 << d for d in dims)

    def piece(rel, chunk, k):
        return gathered.at[owner(rel, core), chunk - MOVED, :, thirds(k)]

    def to_partner(rel, chunk, k):
        remote(piece(rel, chunk, k), piece(rel, chunk, k), mate_send, mate_recv, partner).start()

    def near_to_partner(k, j, chunk):
        remote(near[k].at[j, chunk], mate.at[k, j, chunk], near_send, near_recv, partner).start()

    def gather_one(chunk):
        slot = slot_of(chunk)

        @pl.when(chunk < MOVED)
        def _():
            for k in range(3):
                mine = packed.at[chunk, :, thirds(k)]
                remote(mine, near[k].at[1, chunk], a1s, a1r.at[slot], neighbour[ORDERS[k][0]]).start()
                remote(mine, mate.at[k, 0, chunk], near_send, near_recv, partner).start()
                pltpu.make_async_copy(mine, near[k].at[0, chunk], self_sem).start()

        @pl.when(chunk >= MOVED)
        def _():
            for k in range(3):
                remote(packed.at[chunk, :, thirds(k)], piece(0, chunk, k), a1s, a1r.at[slot], neighbour[ORDERS[k][0]]).start()
            mine = gathered.at[me, chunk - MOVED]
            remote(packed.at[chunk], mine, mate_send, mate_recv, partner).start()
            pltpu.make_async_copy(packed.at[chunk], mine, self_sem).start()

    def gather_two(chunk):
        slot = slot_of(chunk)
        wait_for(packed.at[0], a1r.at[slot])

        @pl.when(chunk < MOVED)
        def _():
            for k in range(3):
                device = neighbour[ORDERS[k][1]]
                remote(packed.at[chunk, :, thirds(k)], near[k].at[2, chunk], a2n, a2r.at[slot], device).start()
                remote(near[k].at[1, chunk], near[k].at[3, chunk], a2n, a2r.at[slot], device).start()
            for k in range(3):
                near_to_partner(k, 1, chunk)

        @pl.when(chunk >= MOVED)
        def _():
            for k in range(3):
                a, b, _ = ORDERS[k]
                remote(packed.at[chunk, :, thirds(k)], piece(0, chunk, k), a2s, a2r.at[slot], neighbour[b]).start()
                remote(piece(offset(a), chunk, k), piece(offset(a), chunk, k), a2s, a2r.at[slot], neighbour[b]).start()
            for k in range(3):
                to_partner(offset(ORDERS[k][0]), chunk, k)

    def gather_three(chunk):
        slot = slot_of(chunk)
        wait_for(packed.at[pl.ds(0, 2)], a2r.at[slot])

        @pl.when(chunk < MOVED)
        def _():
            for k in range(3):
                near_to_partner(k, 2, chunk)
                near_to_partner(k, 3, chunk)

        @pl.when(chunk >= MOVED)
        def _():
            for k in range(3):
                a, b, c = ORDERS[k]
                remote(packed.at[chunk, :, thirds(k)], piece(0, chunk, k), a3s, a3r.at[slot], neighbour[c]).start()
                for rel in (offset(a), offset(b), offset(a, b)):
                    remote(piece(rel, chunk, k), piece(rel, chunk, k), a3s, a3r.at[slot], neighbour[c]).start()
            for k in range(3):
                a, b, c = ORDERS[k]
                to_partner(offset(b), chunk, k)
                to_partner(offset(a, b), chunk, k)

    def gather_four(chunk):
        @pl.when(chunk >= MOVED)
        def _():
            wait_for(packed.at[pl.ds(0, 4)], a3r.at[slot_of(chunk)])
            for k in range(3):
                a, b, c = ORDERS[k]
                for rel in (offset(c), offset(a, c), offset(b, c), offset(a, b, c)):
                    to_partner(rel, chunk, k)

    def at_chunk(chunk, body):
        @pl.when((chunk >= 0) & (chunk < TOTAL))
        def _():
            body(chunk)

    load_own(jnp.int32(0))
    load_own(jnp.int32(1))
    barrier = pltpu.get_barrier_semaphore()
    for k in range(1, 16):
        pl.semaphore_signal(barrier, inc=1, device_id=((me + k) % 16,), device_id_type=MESH)
    pl.semaphore_wait(barrier, 15)
    give_peer(jnp.int32(0))
    give_peer(jnp.int32(1))
    acc[...] = jnp.zeros_like(acc)

    def step(s, _):
        at_chunk(s, pair_stage)

        @pl.when(s + LEAD < TOTAL)
        def _():
            prefetch(s + LEAD)

        @pl.when(s == 0)
        def _():
            for kind in range(4):
                def load_states(i, _, kind=kind):
                    cols = pl.ds(pl.multiple_of(i * CHUNK, CHUNK), CHUNK)
                    for j, dst in enumerate((wv, mv, vv)):
                        pltpu.make_async_copy(states[4 * kind + 1 + j].at[:, cols], dst.at[STARTS[kind] + i], state_sem.at[j]).start()
                    return 0

                lax.fori_loop(0, COUNTS[kind], load_states, 0)

        at_chunk(s - 1, second_stage)
        at_chunk(s - 2, third_stage)

        @pl.when(s == 3)
        def _():
            for j, dst in enumerate((wv, mv, vv)):
                wait_for(dst, state_sem.at[j])

        at_chunk(s - 3, last_stage)
        for kind in range(4):
            @pl.when(s == STARTS[kind] + COUNTS[kind] + 2)
            def _(kind=kind):
                send_norms(kind)

            @pl.when(s == PACK_AT - 2 + STARTS[kind])
            def _(kind=kind):
                take_norms(kind)
        at_chunk(s - PACK_AT - 1, gather_one)
        at_chunk(s - PACK_AT - 2, gather_two)
        at_chunk(s - PACK_AT - 3, gather_three)
        at_chunk(s - PACK_AT - 4, gather_four)
        at_chunk(s - PACK_AT + 2, update)
        at_chunk(s - PACK_AT, pack)
        return 0

    lax.fori_loop(0, TOTAL + PACK_AT + 5, step, 0)

    def drain(chunk, _):
        slot = slot_of(chunk)
        wait_for(peer.at[slot], peer_send.at[slot])
        wait_for(send1.at[slot], s1.at[slot])
        wait_for(recv2.at[slot], s2.at[slot])
        wait_for(recv3.at[slot], s3.at[slot])
        return 0

    lax.fori_loop(TOTAL - SLOTS, TOTAL, drain, 0)
    for kind in range(4):
        wait_for(parts.at[kind, pl.ds(0, 15)], part_send.at[kind])
    wait_for(packed, a1s)
    wait_for(packed, self_sem)
    wait_for(gathered.at[pl.ds(0, 2)], a2s)
    wait_for(mate.at[:, pl.ds(0, 2)], a2n)
    wait_for(gathered.at[pl.ds(0, 4)], a3s)
    for sem in (mate_send, mate_recv):
        wait_for(gathered.at[pl.ds(0, 8)], sem)
    for sem in (near_send, near_recv):
        wait_for(mate, sem)


def wait_for(ref, sem):
    pltpu.make_async_copy(ref, ref, sem).wait()


def in_vmem(x):
    return pltpu.with_memory_space_constraint(x, pltpu.VMEM)


def unpack_part(src, dst, col, rows):
    dst[:, pl.ds(col, THIRD)] = src[0:3, :]
    for row in range(3):
        rows[row:row + 1, :] = src[3:4, row * INNER:(row + 1) * INNER].astype(jnp.float32)
    dst[:, pl.ds(col + THIRD, INNER)] = rows[...].astype(jnp.bfloat16)


class MovedRing:
    def __init__(self, sources, far, outs, buffers):
        self.sources, self.far, self.outs = sources, far, outs
        self.full, self.rows, self.store_sem = buffers
        self.depth = self.full.shape[0]
        self.groups = MOVED // GROUP
        self.steps = 4 * self.groups
        me = lax.axis_index("data")
        self.core = me % 2
        self.bits = ((me // 2) % 2, (me // 4) % 2, (me // 8) % 2)

    def store(self, step):
        slot = lax.rem(step, self.depth)
        j, group = step // self.groups, lax.rem(step, self.groups)
        for i, (_, k, other) in enumerate(self.sources):
            rel = [0, 0, 0]
            for d, bit in zip(ORDERS[k], (j % 2, j // 2, self.far)):
                rel[d] = bit
            shard = self.core + other - 2 * other * self.core
            for d in range(3):
                shard = shard + (2 << d) * (self.bits[d] + rel[d] - 2 * self.bits[d] * rel[d])
            for kind in range(2):
                @pl.when((group >= COUNTS[0] // GROUP) if kind else (group < COUNTS[0] // GROUP))
                def _(kind=kind, i=i, k=k, shard=shard):
                    begin = (shard * COUNTS[kind] + group * GROUP + k - STARTS[kind]) * CHUNK
                    pltpu.make_async_copy(self.full.at[slot, i], self.outs[kind].at[:, pl.ds(pl.multiple_of(begin, CHUNK), CHUNK)],
                                          self.store_sem.at[slot]).start()

    def run(self):
        def body(step, _):
            slot = lax.rem(step, self.depth)

            @pl.when(step >= self.depth)
            def _():
                wait_for(self.full.at[slot], self.store_sem.at[slot])

            j, first = step // self.groups, lax.rem(step, self.groups) * GROUP
            for i, (source, _, _) in enumerate(self.sources):
                for c in range(GROUP):
                    unpack_part(source.at[j, first + c], self.full.at[slot, i], c * PART, self.rows.at[c])
            self.store(step)
            return 0

        lax.fori_loop(0, self.steps, body, 0)

    def drain(self):
        for slot in range(self.depth):
            wait_for(self.full.at[slot], self.store_sem.at[slot])

    @staticmethod
    def scratch(count, depth):
        return [pltpu.VMEM((depth, count, 3, CHUNK), jnp.bfloat16), pltpu.VMEM((GROUP, 3, INNER), jnp.float32), pltpu.SemaphoreType.DMA((depth,))]


def finish_kernel(gathered, near_0, near_1, near_2, mate, wv, mv, vv, *refs):
    outs, refs = refs[:16], refs[16:]
    packed, full, load_sem, store_sem, out_sem = refs[:5]
    units = 16 * ((TOTAL - MOVED) // GROUP)
    sources = [(ref, k, 0) for k, ref in enumerate((near_0, near_1, near_2))]
    sources += [(mate.at[k], k, 1) for k in range(3)]
    moved = MovedRing(sources, 0, (outs[0], outs[4]), refs[5:])
    rows = moved.rows

    def load(unit):
        slot = lax.rem(unit, DEPTH)
        pltpu.make_async_copy(gathered.at[unit % 16, pl.ds((unit // 16) * GROUP, GROUP)], packed.at[slot], load_sem.at[slot]).start()

    def store(unit):
        slot = lax.rem(unit, DEPTH)
        first = (unit // 16) * GROUP + MOVED
        for kind in range(1, 4):
            @pl.when((first >= STARTS[kind]) & (first < STARTS[kind] + COUNTS[kind]))
            def _(kind=kind):
                begin = (unit % 16) * (COUNTS[kind] * CHUNK) + (first - STARTS[kind]) * CHUNK
                cols = pl.ds(pl.multiple_of(begin, CHUNK), GROUP * CHUNK)
                pltpu.make_async_copy(full.at[slot], outs[4 * kind].at[:, cols], store_sem.at[slot]).start()

    def unpack(slot):
        for i in range(GROUP):
            for k in range(3):
                unpack_part(packed.at[slot, i, :, pl.ds(k * THIRD, THIRD)], full.at[slot], k * CHUNK + i * PART, rows.at[k])

    def fill(unit, _):
        load(unit)
        return 0

    lax.fori_loop(0, DEPTH, fill, 0)
    for j, src in enumerate((wv, mv, vv)):
        for kind in range(4):
            def put(i, _, kind=kind, j=j, src=src):
                cols = pl.ds(pl.multiple_of(i * CHUNK, CHUNK), CHUNK)
                pltpu.make_async_copy(src.at[STARTS[kind] + i], outs[4 * kind + 1 + j].at[:, cols], out_sem.at[j]).start()
                return 0

            lax.fori_loop(0, COUNTS[kind], put, 0)

    def step(unit, _):
        slot = lax.rem(unit, DEPTH)
        wait_for(packed.at[slot], load_sem.at[slot])

        @pl.when(unit >= DEPTH)
        def _():
            wait_for(full.at[slot], store_sem.at[slot])

        unpack(slot)
        store(unit)

        @pl.when(unit + DEPTH < units)
        def _():
            load(unit + DEPTH)

        return 0

    lax.fori_loop(0, units, step, 0)
    moved.run()

    def drain(slot, _):
        wait_for(full.at[slot], store_sem.at[slot])
        return 0

    lax.fori_loop(0, DEPTH, drain, 0)
    moved.drain()
    for j, src in enumerate((wv, mv, vv)):
        wait_for(src, out_sem.at[j])


def finish(gathered, near, mate, new_states):
    f32, bf16 = jnp.float32, jnp.bfloat16
    dma = pltpu.SemaphoreType.DMA
    any_space = pl.BlockSpec(memory_space=pl.ANY)
    shapes = []
    for count in COUNTS:
        shapes += [jax.ShapeDtypeStruct((3, 16 * count * CHUNK), bf16)] + [jax.ShapeDtypeStruct((3, count * CHUNK), f32)] * 3
    return pl.pallas_call(
        finish_kernel,
        out_shape=tuple(shapes),
        in_specs=[any_space] + [pl.BlockSpec(memory_space=pltpu.VMEM)] * 7,
        out_specs=(any_space,) * 16,
        scratch_shapes=[
            pltpu.VMEM((DEPTH, GROUP, 4, PACKED), bf16), pltpu.VMEM((DEPTH, 3, GROUP * CHUNK), bf16),
            dma((DEPTH,)), dma((DEPTH,)), dma((3,)),
        ] + MovedRing.scratch(6, RING),
        compiler_params=pltpu.CompilerParams(vmem_limit_bytes=LAST_VMEM),
        cost_estimate=pl.CostEstimate(flops=10 ** 12, bytes_accessed=10 ** 8, transcendentals=0),
        name="finish",
    )(pltpu.with_memory_space_constraint(gathered, pltpu.HBM), *[in_vmem(x) for x in (*near, mate, *new_states)])


def far_kernel(other, *refs):
    arrays, outs, buffers = refs[:3], refs[5:7], refs[7:]
    ring = MovedRing([(ref, k, other) for k, ref in enumerate(arrays)], 1, outs, buffers)
    ring.run()
    ring.drain()


def finish_far(far, other, copies):
    any_space = pl.BlockSpec(memory_space=pl.ANY)
    return pl.pallas_call(
        functools.partial(far_kernel, other),
        out_shape=tuple(jax.ShapeDtypeStruct(x.shape, x.dtype) for x in copies),
        in_specs=[pl.BlockSpec(memory_space=pltpu.VMEM)] * 3 + [any_space] * 2,
        out_specs=(any_space,) * 2,
        scratch_shapes=MovedRing.scratch(3, FAR_RING),
        input_output_aliases={3: 0, 4: 1},
        compiler_params=pltpu.CompilerParams(vmem_limit_bytes=FAR_VMEM),
        cost_estimate=pl.CostEstimate(flops=10 ** 11, bytes_accessed=10 ** 7, transcendentals=0),
    )(*far, *copies)


def optimizer_step(blocks):
    f32, bf16 = jnp.float32, jnp.bfloat16
    dma = pltpu.SemaphoreType.DMA
    any_space = pl.BlockSpec(memory_space=pl.ANY)
    operands = []
    for kind in KINDS:
        grad, weight, first_mom, second_mom = blocks[4 * kind:4 * kind + 4]
        operands += [grad.reshape(grad.shape[1:]), weight, first_mom, second_mom]
    part = pltpu.VMEM((4, MOVED, 4, THIRD), bf16)
    state = pltpu.VMEM((TOTAL, 3, CHUNK), f32)
    vmem_space = pl.BlockSpec(memory_space=pltpu.VMEM)
    return pl.pallas_call(
        step_kernel,
        out_shape=(pltpu.HBM((16, TOTAL - MOVED, 4, PACKED), bf16), part, part, part, pltpu.VMEM((3,) + part.shape, bf16), state, state, state),
        in_specs=[any_space] * 16,
        out_specs=(any_space,) + (vmem_space,) * 7,
        scratch_shapes=[
            pltpu.VMEM((SLOTS, 8, 3, CHUNK), bf16), pltpu.VMEM((SLOTS, 8, 3, CHUNK), bf16), pltpu.VMEM((8, 3, INNER), f32),
            pltpu.VMEM((SLOTS, 3, 4, 1, CHUNK), f32), pltpu.VMEM((SLOTS, 3, 4, 1, CHUNK), f32),
            pltpu.VMEM((SLOTS, 3, 4, 1, CHUNK), f32), pltpu.VMEM((SLOTS, 3, 2, 1, CHUNK), f32), pltpu.VMEM((SLOTS, 3, 1, 1, CHUNK), f32),
            pltpu.VMEM((TOTAL, 3, 1, CHUNK), f32),
            pltpu.VMEM((4, 6, 1, INNER), f32), pltpu.VMEM((4, 8, 128), f32), pltpu.VMEM((4, 16, 8, 128), f32), pltpu.VMEM((4, 3, 1, INNER), f32),
            pltpu.VMEM((3, 4, INNER), f32), pltpu.VMEM((TOTAL, 4, PACKED), bf16),
            dma((SLOTS, 3)), dma((SLOTS,)), dma((SLOTS, 3)),
            dma((SLOTS,)), dma((SLOTS,)), dma((SLOTS,)), dma((SLOTS,)), dma((SLOTS,)), dma((SLOTS,)),
            dma((3,)), dma((4,)), dma((4,)),
            dma, dma, dma, dma((SLOTS,)), dma((SLOTS,)), dma((SLOTS,)), dma, dma, dma, dma, dma, dma,
        ],
        compiler_params=pltpu.CompilerParams(collective_id=0, has_side_effects=True, vmem_limit_bytes=STEP_VMEM),
        name="lamb_step",
    )(*operands)


def solution(mesh):
    grad_spec = P("data", None, None)
    shard_spec = P(None, "data")
    full_spec = P(None, None)

    def device_step(*blocks):
        gathered, *near_mate = optimizer_step(blocks)
        near, mate, new_states = near_mate[:3], near_mate[3], near_mate[4:]
        far = []
        for k in range(3):
            far.append(in_vmem(lax.ppermute(near[k], "data", [(i, i ^ (2 << ORDERS[k][2])) for i in range(16)])))
        outs = list(finish(gathered, near, mate, new_states))
        far_mate = []
        for k in range(3):
            far_mate.append(in_vmem(lax.ppermute(far[k], "data", [(i, i ^ 1) for i in range(16)])))
        copies = (outs[0], outs[4])
        copies = finish_far(far, 0, copies)
        outs[0], outs[4] = finish_far(far_mate, 1, copies)
        results = [None] * 16
        for slot, kind in enumerate(KINDS):
            results[4 * kind:4 * kind + 4] = outs[4 * slot:4 * slot + 4]
        return tuple(results)

    return jax.shard_map(device_step, mesh=mesh, in_specs=(grad_spec, shard_spec, shard_spec, shard_spec) * 4, out_specs=(full_spec, shard_spec, shard_spec, shard_spec) * 4, check_vma=False)
```
